256 devices in a mesh: row: 8 (over x_lo, y), col: 32 (over z, x_hi, core).
Axes of the slice: x: 4 (x_hi: 2, x_lo: 2; x = x_hi * 2 + x_lo), y: 4, z: 8, core: 2. Of those that a mesh axis runs over, the one named last changes fastest.
Arguments:
- pair_rep: bfloat16 [1024, 1024, 128], P('row', 'col'), may hold values from -6 to 6
- ln_gain: float32 [128], replicated, may hold values from 0.1 to 1.9
- ln_shift: float32 [128], replicated, may hold values from -3 to 3
- w_proj: bfloat16 [128, 512], replicated, may hold values from -0.5 to 0.5
- gate_bias: float32 [128], replicated, may hold values from -4 to 4
- w_bias: bfloat16 [128, 4], replicated, may hold values from -11 to 11
- w_out: bfloat16 [128, 128], replicated, may hold values from -0.5 to 0.5
- out_bias: float32 [128], replicated, may hold values from -3 to 3
- block_valid: int32 [8], replicated, may hold values from 0 to 1, as said below
Outputs:
- pair_out: bfloat16 [1024, 1024, 128], P('row', 'col')
The draws below stay inside these ranges and needn't reach their ends.
Inputs may be any that keep to these rules, and one draw needn't show every extreme that they name: block_valid[b] is 1 when residues b * 128 to (b + 1) * 128 - 1 are present and 0 when they are padding; blocks 0 and 4 are always present, and at least one other block is always padding.
All inputs are finite; a program needn't handle non-finite values.
Results may differ from the reference program's by a relative error of at most 0.0082.
Values may be sent and summed in bfloat16 or wider, within the bound.
A program may use at most 192 MiB of HBM per device.

```python
import jax
import jax.numpy as jnp
from jax import lax

C = 128
H = 4
HD = 32
RES = 1024
NBLK = 8


def draw_w_bias(key, part):
    base = jnp.clip(jax.random.normal(key, (C, H), jnp.float32), -4.0, 4.0) * 0.13
    return base.astype(jnp.bfloat16)


def draw_block_valid(key, part):
    places = jnp.arange(NBLK, dtype=jnp.int32)
    levels = jax.random.randint(key, (NBLK,), 0, 2, dtype=jnp.int32)
    bits = jnp.where(levels > 0, 1, 0).astype(jnp.int32)
    bits = jnp.where((places == 0) | (places == NBLK // 2), 1, bits)
    if NBLK >= 3:
        candidate = jax.random.randint(jax.random.fold_in(key, 7), (), 1, NBLK - 1, dtype=jnp.int32)
        padded = jnp.where(candidate == NBLK // 2, NBLK - 1, candidate).astype(jnp.int32)
        bits = jnp.where(places == padded, 0, bits)
    return bits.astype(jnp.int32)


def level_of(own_key, dims, pieces, low, high):
    level = 1.0
    for dim, blocks in pieces:
        steps = jax.random.uniform(jax.random.fold_in(jax.random.fold_in(own_key, 6), dim), (blocks,), jnp.float32, low / len(pieces), high / len(pieces))
        level = level * jnp.repeat(jnp.exp(steps), dims[dim] // blocks).reshape((-1,) + (1,) * (len(dims) - 1 - dim))
    return level


def noise(rng, dims, deviation, most, split=(), kind=jnp.bfloat16):
    gain = level_of(rng, dims, split, -0.22, 0.18) if split else 1.0
    values = jax.random.normal(rng, dims, jnp.float32) * deviation * gain
    return jnp.minimum(jnp.maximum(values, -most), most).astype(kind)


def setup_inputs(seed: int = 0) -> dict:
    arg_keys = jax.random.split(jax.random.key(seed), 10)
    return {
        "pair_rep": noise(arg_keys[0], (RES, RES, C), 1.0, 6.0, ((0, 8), (1, 32))),
        "ln_gain": jnp.clip(1.0 + 0.18 * jax.random.normal(arg_keys[1], (C,), jnp.float32), 0.1, 1.9),
        "ln_shift": noise(arg_keys[2], (C,), 0.5, 3.0, (), jnp.float32),
        "w_proj": noise(arg_keys[3], (C, 4 * H * HD), C ** -0.5, 0.5),
        "gate_bias": noise(arg_keys[4], (H * HD,), 1.0, 4.0, (), jnp.float32),
        "w_bias": draw_w_bias(jax.random.fold_in(arg_keys[9], 71), 0),
        "w_out": noise(arg_keys[6], (H * HD, C), (H * HD) ** -0.5, 0.5),
        "out_bias": noise(arg_keys[7], (C,), 0.5, 3.0, (), jnp.float32),
        "block_valid": draw_block_valid(jax.random.fold_in(arg_keys[9], 71), 0),
    }


def layer_norm(values, ln_gain, ln_shift):
    widened = values.astype(jnp.float32)
    average = lax.optimization_barrier(jnp.mean(widened, axis=-1, keepdims=True))
    spread = lax.optimization_barrier(jnp.mean((widened - average) ** 2, axis=-1, keepdims=True))
    return ((widened - average) * lax.rsqrt(spread + 1e-05) * ln_gain + ln_shift).astype(jnp.bfloat16)

def residue_valid(block_valid, residues):
    blocks = block_valid.shape[0]
    block_width = residues // blocks
    owner = jnp.arange(residues, dtype=jnp.int32) // block_width
    matches = (owner[:, None] == jnp.arange(blocks, dtype=jnp.int32)[None, :]).astype(jnp.float32)
    return lax.optimization_barrier(jnp.sum(matches * block_valid.astype(jnp.float32)[None, :], axis=1))

def reference(pair_rep, ln_gain, ln_shift, w_proj, gate_bias, w_bias, w_out, out_bias, block_valid):
    residues = pair_rep.shape[0]
    inner = H * HD
    validity = residue_valid(block_valid, residues)
    normed = lax.map(lambda row_in: layer_norm(row_in, ln_gain, ln_shift), pair_rep)
    bias_rows = lax.map(lambda row_in: jnp.dot(row_in, w_bias, preferred_element_type=jnp.float32), normed)
    bias_t = jnp.transpose(bias_rows, (2, 1, 0))

    def column(index):
        column_in = lax.dynamic_index_in_dim(normed, index, 1, keepdims=False)
        pair_col = lax.dynamic_index_in_dim(pair_rep, index, 1, keepdims=False)
        projected = jnp.dot(column_in, w_proj, preferred_element_type=jnp.float32)
        queries = (projected[:, :inner] * HD ** (-0.5)).astype(jnp.bfloat16)
        key_rows = projected[:, inner:2 * inner].astype(jnp.bfloat16)
        values = projected[:, 2 * inner:3 * inner].astype(jnp.bfloat16)
        gate_act = jax.nn.sigmoid(projected[:, 3 * inner:] + gate_bias)
        query_heads = queries.reshape(residues, H, HD).astype(jnp.float32)
        key_heads = key_rows.reshape(residues, H, HD).astype(jnp.float32)
        value_heads = values.reshape(residues, H, HD).astype(jnp.float32)
        scores = jnp.einsum('ihd,khd->hik', query_heads, key_heads) + bias_t
        scores = jnp.where(validity[None, None, :] > 0, scores, jnp.float32(-1e+30))
        row_max = lax.optimization_barrier(jnp.max(scores, axis=-1, keepdims=True))
        weights = jnp.exp(scores - row_max) * validity[None, None, :]
        denominator = lax.optimization_barrier(jnp.sum(weights, axis=-1))
        rounded = weights.astype(jnp.bfloat16).astype(jnp.float32)
        mixed = jnp.einsum('hik,khd->ihd', rounded, value_heads) / jnp.transpose(denominator)[:, :, None]
        attended = mixed.reshape(residues, inner).astype(jnp.bfloat16)
        gated_rows = (gate_act * attended.astype(jnp.float32)).astype(jnp.bfloat16)
        update = jnp.dot(gated_rows, w_out, preferred_element_type=jnp.float32) + out_bias
        col_valid = lax.dynamic_index_in_dim(validity, index, 0, keepdims=False)
        update = update * (validity * col_valid)[:, None]
        return (pair_col.astype(jnp.float32) + update).astype(jnp.bfloat16)
    results = lax.map(column, jnp.arange(residues, dtype=jnp.int32))
    return jnp.transpose(results, (1, 0, 2))
```

```python
import jax
import jax.numpy as jnp
from jax import lax
from jax.experimental import pallas as pl
from jax.experimental.pallas import tpu as pltpu
from jax.sharding import PartitionSpec as P

H = 4
HD = 32
C = 128
ROWS = 8
COLS = 32
BLK = 128
JW = 4
BROWS = H * 32 + 8
COLOR_Z = (0, 72)
COLOR_Y = (72, 96)
COLOR_X = (96, 136)
MESH = pl.DeviceIdType.MESH
F32 = jnp.float32
BF16 = jnp.bfloat16
NEG = -1e30


def dot_nt(a, b):
    return lax.dot_general(a, b, (((1,), (1,)), ((), ())), preferred_element_type=F32)


def dot_nn(a, b):
    return lax.dot_general(a, b, (((1,), (0,)), ((), ())), preferred_element_type=F32)


def layer_norm(x, gain, shift):
    average = jnp.mean(x, axis=-1, keepdims=True)
    centred = x - average
    spread = jnp.mean(centred * centred, axis=-1, keepdims=True)
    return (centred * lax.rsqrt(spread + 1e-05) * gain + shift).astype(BF16)


def bias_kernel(x_ref, gain_ref, shift_ref, wb_ref, blk_ref, n_s, b_s):
    col = lax.axis_index("col")

    def norm(step, carry):
        x = x_ref[pl.ds(step * 16, 16), :, :].astype(F32).reshape(512, C)
        n_s[pl.ds(pl.multiple_of(step * 512, 512), 512), :] = layer_norm(
            x, gain_ref[...], shift_ref[...]
        ).astype(F32)
        return carry

    lax.fori_loop(0, 8, norm, 0)
    lanes = lax.broadcasted_iota(jnp.int32, (8, BLK), 1)
    first = lax.rem(col, 4) * 32
    centres = jnp.zeros((8, BLK), F32)
    for i in range(32):
        rows = n_s[pl.ds(i, BLK, stride=32), :].astype(BF16)
        part = dot_nt(wb_ref[...], rows)
        centre = jnp.max(part, axis=-1, keepdims=True).astype(BF16).astype(F32)
        part = part - centre
        for h in range(H):
            b_s[h * 32 + i : h * 32 + i + 1, :] = part[h : h + 1, :]
        centres = jnp.where(lanes == first + i, centre, centres)
    blk_ref[0 : H * 32, :] = b_s[...].astype(BF16)
    blk_ref[H * 32 :, :] = centres.astype(BF16)


def local_bias(x, gain, shift, wb):
    return pl.pallas_call(
        bias_kernel,
        out_shape=jax.ShapeDtypeStruct((BROWS, BLK), BF16),
        scratch_shapes=[pltpu.VMEM((4096, C), F32), pltpu.VMEM((H * 32, BLK), F32)],
        compiler_params=pltpu.CompilerParams(vmem_limit_bytes=24 * 1024 * 1024),
        name="local_bias",
    )(x, gain, shift, wb)


def exchange_kernel(
    x_ref, blk_ref, o_ref, bg_ref,
    a_send, a_recv, z_send, z_recv, y_send, y_recv, x_send, x_recv,
    rz_send, rz_recv, ry_send, ry_recv, rx_send, rx_recv,
    dz_send, dz_recv, dy_send, dy_recv, dx_send, dx_recv, local_sem,
):
    row = lax.axis_index("row")
    col = lax.axis_index("col")
    xl, y = row // 4, lax.rem(row, 4)
    z, xh, core = col // 4, lax.rem(col // 2, 2), lax.rem(col, 2)
    x = xh * 2 + xl

    def device(x_, y_, z_, core_):
        return {"row": lax.rem(x_, 2) * 4 + y_, "col": z_ * 4 + (x_ // 2) * 2 + core_}

    def block(x_, y_, z_, core_, color):
        return bg_ref.at[lax.rem(x_, 2), y_, z_, x_ // 2, core_, pl.ds(color[0], color[1] - color[0]), :]

    planes = (
        (16, x * 4 + y, lambda p: (p // 4, lax.rem(p, 4), z), COLOR_Z, z_send, z_recv),
        (32, x * 8 + z, lambda p: (p // 8, y, lax.rem(p, 8)), COLOR_Y, y_send, y_recv),
        (32, y * 8 + z, lambda p: (x, p // 8, lax.rem(p, 8)), COLOR_X, x_send, x_recv),
    )

    barrier = pltpu.get_barrier_semaphore()
    for count, mine, at, color, send, recv in planes:
        def greet(d, carry, count=count, mine=mine, at=at):
            px, py, pz = at(lax.rem(mine + d, count))
            pl.semaphore_signal(
                barrier, inc=1, device_id=device(px, py, pz, core), device_id_type=MESH
            )
            return carry

        lax.fori_loop(1, count, greet, 0)
    pl.semaphore_signal(barrier, inc=1, device_id=device(x, y, z, 1 - core), device_id_type=MESH)
    pl.semaphore_wait(barrier, 78)

    def plane_copy(plane, peer, sender):
        count, mine, at, color, send, recv = plane
        px, py, pz = at(peer)
        sx, sy, sz = at(sender)
        return pltpu.make_async_remote_copy(
            src_ref=blk_ref.at[pl.ds(color[0], color[1] - color[0]), :],
            dst_ref=block(sx, sy, sz, core, color),
            send_sem=send.at[peer],
            recv_sem=recv.at[sender],
            device_id=device(px, py, pz, core),
            device_id_type=MESH,
        )

    own = pltpu.make_async_copy(blk_ref, bg_ref.at[xl, y, z, xh, core], local_sem.at[0])
    own.start()
    for plane in planes:
        count, mine = plane[0], plane[1]

        def start(d, carry, plane=plane, count=count, mine=mine):
            plane_copy(plane, lax.rem(mine + d, count), mine).start()
            return carry

        lax.fori_loop(1, count, start, 0)

    def column_copy(peer, sender):
        return pltpu.make_async_remote_copy(
            src_ref=x_ref.at[:, peer],
            dst_ref=o_ref.at[sender],
            send_sem=a_send.at[peer],
            recv_sem=a_recv.at[sender],
            device_id={"row": peer, "col": col},
            device_id_type=MESH,
        )

    def start_column(d, carry):
        column_copy(lax.rem(row + d, ROWS), row).start()
        return carry

    lax.fori_loop(1, ROWS, start_column, 0)
    keep = pltpu.make_async_copy(x_ref.at[:, row], o_ref.at[row], local_sem.at[1])
    keep.start()

    def z_unit(p, half):
        rows = slice(None) if half is None else pl.ds(half, 1)
        return bg_ref.at[rows, :, p, :, core, pl.ds(COLOR_Z[0], COLOR_Z[1] - COLOR_Z[0]), :]

    def y_unit(p, half):
        rows = slice(None) if half is None else pl.ds(half, 1)
        return bg_ref.at[rows, p, :, :, core, pl.ds(COLOR_Y[0], COLOR_Y[1] - COLOR_Y[0]), :]

    def x_unit(p, half):
        rows = slice(None) if half is None else pl.ds(half * 2, 2)
        return bg_ref.at[lax.rem(p, 2), rows, :, p // 2, core, pl.ds(COLOR_X[0], COLOR_X[1] - COLOR_X[0]), :]

    rings = (
        (8, z, z_unit, lambda p: device(x, y, p, core), rz_send, rz_recv, dz_send, dz_recv),
        (4, x, x_unit, lambda p: device(p, y, z, core), rx_send, rx_recv, dx_send, dx_recv),
        (4, y, y_unit, lambda p: device(x, p, z, core), ry_send, ry_recv, dy_send, dy_recv),
    )

    def hop(ring, way, step):
        size, mine, unit, at, send, recv, _, _ = ring
        last = size // 2
        sign = 1 if way == 0 else -1
        half = way if step == last else None
        moved = lax.rem(mine - sign * (step - 1) + size, size)
        return pltpu.make_async_remote_copy(
            src_ref=unit(moved, half),
            dst_ref=unit(moved, half),
            send_sem=send.at[way, step - 1],
            recv_sem=recv.at[way, step - 1],
            device_id=at(lax.rem(mine + sign + size, size)),
            device_id_type=MESH,
        )

    def arrived(ring, way, step):
        size, mine, unit, at, send, recv, _, _ = ring
        last = size // 2
        sign = 1 if way == 0 else -1
        half = way if step == last else None
        got = lax.rem(mine - sign * step + 2 * size, size)
        return pltpu.make_async_remote_copy(
            src_ref=unit(got, half),
            dst_ref=unit(got, half),
            send_sem=send.at[way, step - 1],
            recv_sem=recv.at[way, step - 1],
            device_id=at(lax.rem(mine + sign + size, size)),
            device_id_type=MESH,
        )

    def across(ring, place):
        size, mine, unit, at, _, _, send, recv = ring
        return pltpu.make_async_remote_copy(
            src_ref=unit(place, None),
            dst_ref=unit(place, None),
            send_sem=send.at[place],
            recv_sem=recv.at[place],
            device_id=device(x, y, z, 1 - core),
            device_id_type=MESH,
        )

    own.wait()
    for plane, ring in zip((planes[0], planes[2], planes[1]), rings):
        pass
    order = ((planes[0], rings[0]), (planes[1], rings[2]), (planes[2], rings[1]))
    for plane, ring in order:
        count, mine = plane[0], plane[1]

        def take(d, carry, plane=plane, count=count, mine=mine):
            peer = lax.rem(mine + d, count)
            plane_copy(plane, peer, peer).wait_recv()
            return carry

        lax.fori_loop(1, count, take, 0)
        hop(ring, 0, 1).start()
        hop(ring, 1, 1).start()
        across(ring, ring[1]).start()

    for step in (1, 2, 3, 4):
        for plane, ring in order:
            size, mine = ring[0], ring[1]
            last = size // 2
            if step > last:
                continue
            for way in (0, 1):
                arrived(ring, way, step).wait_recv()
                if step < last:
                    hop(ring, way, step + 1).start()
                    sign = 1 if way == 0 else -1
                    across(ring, lax.rem(mine - sign * step + size, size)).start()
            if step == last:
                across(ring, lax.rem(mine + last, size)).start()

    for plane in planes:
        count, mine = plane[0], plane[1]

        def sent(d, carry, plane=plane, count=count, mine=mine):
            plane_copy(plane, lax.rem(mine + d, count), mine).wait_send()
            return carry

        lax.fori_loop(1, count, sent, 0)
    for plane, ring in order:
        size, mine = ring[0], ring[1]
        for way in (0, 1):
            for step in range(1, size // 2 + 1):
                hop(ring, way, step).wait_send()
        for d in range(size):
            across(ring, d).wait_send()

    def columns_done(d, carry):
        peer = lax.rem(row + d, ROWS)
        column_copy(peer, row).wait_send()
        column_copy(peer, peer).wait_recv()
        return carry

    lax.fori_loop(1, ROWS, columns_done, 0)
    keep.wait()
    for plane, ring in order:
        size, unit, recv = ring[0], ring[2], ring[7]

        for d in range(size):
            other = ring_other(bg_ref, ring, d, core)
            pltpu.make_async_remote_copy(
                src_ref=other,
                dst_ref=other,
                send_sem=ring[6].at[d],
                recv_sem=recv.at[d],
                device_id=device(x, y, z, 1 - core),
                device_id_type=MESH,
            ).wait_recv()


def ring_other(bg_ref, ring, place, core):
    size = ring[0]
    if size == 8:
        return bg_ref.at[:, :, place, :, 1 - core, pl.ds(COLOR_Z[0], COLOR_Z[1] - COLOR_Z[0]), :]
    if ring[2].__name__ == "y_unit":
        return bg_ref.at[:, place, :, :, 1 - core, pl.ds(COLOR_Y[0], COLOR_Y[1] - COLOR_Y[0]), :]
    return bg_ref.at[
        place % 2, :, :, place // 2, 1 - core, pl.ds(COLOR_X[0], COLOR_X[1] - COLOR_X[0]), :
    ]


def exchange(x, blk):
    dma = pltpu.SemaphoreType.DMA
    return pl.pallas_call(
        exchange_kernel,
        out_shape=(
            jax.ShapeDtypeStruct((ROWS, BLK, JW, C), BF16),
            jax.ShapeDtypeStruct((2, 4, 8, 2, 2, BROWS, BLK), BF16),
        ),
        in_specs=[pl.BlockSpec(memory_space=pl.ANY), pl.BlockSpec(memory_space=pltpu.VMEM)],
        out_specs=(pl.BlockSpec(memory_space=pl.ANY), pl.BlockSpec(memory_space=pl.ANY)),
        scratch_shapes=[
            dma((8,)), dma((8,)), dma((16,)), dma((16,)), dma((32,)), dma((32,)), dma((32,)), dma((32,)),
            dma((2, 4)), dma((2, 4)), dma((2, 2)), dma((2, 2)), dma((2, 2)), dma((2, 2)),
            dma((8,)), dma((8,)), dma((4,)), dma((4,)), dma((4,)), dma((4,)), dma((2,)),
        ],
        compiler_params=pltpu.CompilerParams(collective_id=0, has_side_effects=True),
        name="exchange",
    )(x.reshape(BLK, ROWS, JW, C), blk)


def return_kernel(y_ref, o_ref, send, recv, local_sem):
    row = lax.axis_index("row")
    barrier = pltpu.get_barrier_semaphore()
    for d in range(1, ROWS):
        pl.semaphore_signal(
            barrier, inc=1, device_id={"row": lax.rem(row + d, ROWS)}, device_id_type=MESH
        )
    pl.semaphore_wait(barrier, ROWS - 1)

    def copy(peer, sender):
        return pltpu.make_async_remote_copy(
            src_ref=y_ref.at[peer],
            dst_ref=o_ref.at[:, sender],
            send_sem=send.at[peer],
            recv_sem=recv.at[sender],
            device_id={"row": peer},
            device_id_type=MESH,
        )

    for d in range(1, ROWS):
        copy(lax.rem(row + d, ROWS), row).start()
    keep = pltpu.make_async_copy(y_ref.at[row], o_ref.at[:, row], local_sem)
    keep.start()
    for d in range(1, ROWS):
        peer = lax.rem(row + d, ROWS)
        copy(peer, row).wait_send()
        copy(peer, peer).wait_recv()
    keep.wait()


def send_back(y):
    dma = pltpu.SemaphoreType.DMA
    return pl.pallas_call(
        return_kernel,
        out_shape=jax.ShapeDtypeStruct((BLK, ROWS, JW, C), BF16),
        in_specs=[pl.BlockSpec(memory_space=pl.ANY)],
        out_specs=pl.BlockSpec(memory_space=pl.ANY),
        scratch_shapes=[dma((8,)), dma((8,)), dma],
        compiler_params=pltpu.CompilerParams(collective_id=1, has_side_effects=True),
        name="send_back",
    )(y)


def attend_kernel(
    valid_ref, x_ref, bg_ref, gain_ref, shift_ref, wp_ref, gb_ref, wo_ref, ob_ref, out_ref,
    q_s, k_s, v_s, g_s, tq, tk, tv, tg, p_s, acc_s, u_s, mx_s, top_s, idx_s,
):
    col = lax.axis_index("col")
    present = valid_ref[col // 4]

    def place(b, count):
        idx_s[count] = b
        return count + valid_ref[b]

    n = lax.fori_loop(0, 8, place, 0)
    idx_s[n] = 0
    pairs = (n + 1) // 2
    lanes = lax.broadcasted_iota(jnp.int32, (BLK, C), 1)
    subs = lax.broadcasted_iota(jnp.int32, (BLK, C), 0)

    @pl.when(present == 0)
    def _():
        out_ref[...] = x_ref[...]

    @pl.when(present != 0)
    def _():
        top_s[...] = jnp.zeros_like(top_s)

        def prepare(s, carry):
            r = idx_s[s]
            tok = pl.multiple_of(r * 512, 512)
            x = x_ref[pl.ds(tok, 512), :].astype(F32)
            normed = layer_norm(x, gain_ref[...], shift_ref[...])
            proj = dot_nn(normed, wp_ref[...])
            q = (proj[:, :C] * (HD ** -0.5)).astype(BF16)
            k = proj[:, C : 2 * C].astype(BF16)
            tq[...] = q.astype(F32)
            tk[...] = k.astype(F32)
            tv[...] = proj[:, 2 * C : 3 * C]
            tg[...] = jax.nn.sigmoid(proj[:, 3 * C :] + gb_ref[...])
            heads = (
                lax.broadcasted_iota(jnp.int32, (C, C), 0) // HD
                == lax.broadcasted_iota(jnp.int32, (C, C), 1) // HD
            ).astype(BF16)
            q2 = dot_nn(q * q, heads)
            k2 = dot_nn(k * k, heads)
            top_s[0] = jnp.maximum(top_s[0], jnp.max(q2.reshape(64, 8, C), axis=0))
            top_s[1] = jnp.maximum(top_s[1], jnp.max(k2.reshape(64, 8, C), axis=0))

            tiles = []
            high = jnp.full((8, BLK), NEG, F32)
            for b in range(8):
                part = bg_ref[b // 4, b % 4, r, 0, 0, H * 32 :, :].astype(F32)
                for q4 in range(1, 4):
                    part = part + bg_ref[b // 4, b % 4, r, q4 // 2, q4 % 2, H * 32 :, :].astype(F32)
                ok = valid_ref[b] > 0
                tiles.append(jnp.where(ok, part, 0.0))
                high = jnp.maximum(high, jnp.where(ok, part, NEG))
            tiles.append(-high)
            tiles.append(jnp.full((8, BLK), NEG, F32))
            tiles.append(jnp.zeros((48, BLK), F32))
            turned = jnp.concatenate(tiles, axis=0).T
            at = pl.multiple_of(s * BLK, BLK)
            it = s // 2
            sub = pl.multiple_of(lax.rem(s, 2) * BLK, BLK)
            k_pick = jnp.where((lanes // 8 == r) | (lanes // 8 == 8), 1.0, 0.0).astype(BF16)
            for j in range(JW):
                qj = tq[pl.ds(j, BLK, stride=JW), :]
                vj = tv[pl.ds(j, BLK, stride=JW), :]
                k_s[j, pl.ds(at, BLK), 0:C] = tk[pl.ds(j, BLK, stride=JW), :].astype(BF16)
                k_s[j, pl.ds(at, BLK), C : 2 * C] = k_pick
                g_s[j, pl.ds(at, BLK), :] = tg[pl.ds(j, BLK, stride=JW), :]
                for h in range(H):
                    mine = lanes // HD == h
                    q_s[j, it, h, pl.ds(sub, BLK), 0:C] = jnp.where(mine, qj, 0.0).astype(BF16)
                    v_s[j, it, h, pl.ds(sub, BLK), 0:C] = jnp.where(mine, vj, 0.0).astype(BF16)
                    v_s[j, it, h, pl.ds(sub, BLK), C : 2 * C] = jnp.where(mine, 1.0, 0.0).astype(BF16)
            for h in range(H):
                e = jnp.where(
                    ((lax.rem(lanes, 8) == h) & (lanes < 72)) | (lanes == 72), turned, 0.0
                ).astype(BF16)
                for j in range(JW):
                    q_s[j, it, h, pl.ds(sub, BLK), C : 2 * C] = e
            return carry

        lax.fori_loop(0, n, prepare, 0)

        @pl.when(lax.rem(n, 2) == 1)
        def _():
            at = pl.multiple_of(n * BLK, BLK)
            it = n // 2
            zero = jnp.zeros((BLK, C), BF16)
            for j in range(JW):
                k_s[j, pl.ds(at, BLK), 0:C] = zero
                k_s[j, pl.ds(at, BLK), C : 2 * C] = jnp.where(lanes == 72, 1.0, 0.0).astype(BF16)
                for h in range(H):
                    v_s[j, it, h, BLK : 2 * BLK, :] = jnp.zeros((BLK, 2 * C), BF16)
                    q_s[j, it, h, BLK : 2 * BLK, :] = jnp.zeros((BLK, 2 * C), BF16)

        bound = jnp.max(jnp.max(top_s[0], axis=0, keepdims=True) * jnp.max(top_s[1], axis=0, keepdims=True))

        def scores(j, it, kt, h):
            s = dot_nt(
                q_s[j, it, h], k_s[j, pl.ds(pl.multiple_of(kt * 256, 256), 256), :]
            )
            rows = []
            for a in range(2):
                ri = idx_s[it * 2 + a]
                parts = []
                for b in range(2):
                    rk = idx_s[kt * 2 + b]
                    bias = bg_ref[rk // 4, lax.rem(rk, 4), ri, :, :, h * 32 : h * 32 + 32, :]
                    parts.append(
                        s[a * BLK : (a + 1) * BLK, b * BLK : (b + 1) * BLK]
                        + bias.reshape(BLK, BLK).astype(F32)
                    )
                rows.append(jnp.concatenate(parts, axis=1))
            return jnp.concatenate(rows, axis=0)

        def tile(j, it, shifted):
            acc_s[...] = jnp.zeros_like(acc_s)

            def over_keys(kt, carry):
                for h in range(H):
                    s = scores(j, it, kt, h)
                    if shifted:
                        s = s - mx_s[h][:, 0:1]
                    p_s[:, h * 256 : (h + 1) * 256] = jnp.exp(s).astype(BF16)
                acc_s[...] += dot_nn(p_s[...], v_s[j, kt].reshape(H * 256, 256))
                return carry

            lax.fori_loop(0, pairs, over_keys, 0)

        def finish(j, it):
            base = pl.multiple_of(it * 256, 256)
            mixed = (acc_s[:, 0:C] / acc_s[:, C : 2 * C]).astype(BF16).astype(F32)
            gated = (g_s[j, pl.ds(base, 256), :] * mixed).astype(BF16)
            update = dot_nn(gated, wo_ref[...]) + ob_ref[...]
            for a in range(2):
                ri = idx_s[it * 2 + a]

                @pl.when(it * 2 + a < n)
                def _():
                    u_s[pl.ds(ri * 512 + j, BLK, stride=JW), :] = update[a * BLK : (a + 1) * BLK]

        def over_tiles(step, carry):
            j, it = step // pairs, lax.rem(step, pairs)
            tile(j, it, False)
            finish(j, it)
            return carry

        def over_tiles_shifted(step, carry):
            j, it = step // pairs, lax.rem(step, pairs)
            mx_s[...] = jnp.full_like(mx_s, NEG)

            def highest(kt, inner):
                for h in range(H):
                    top = jnp.max(scores(j, it, kt, h), axis=-1, keepdims=True)
                    mx_s[h] = jnp.maximum(mx_s[h], top)
                return inner

            lax.fori_loop(0, pairs, highest, 0)
            tile(j, it, True)
            finish(j, it)
            return carry

        @pl.when(bound <= 3000.0)
        def _():
            lax.fori_loop(0, pairs * JW, over_tiles, 0)

        @pl.when(jnp.logical_not(bound <= 3000.0))
        def _():
            lax.fori_loop(0, pairs * JW, over_tiles_shifted, 0)

        def write(r, carry):
            tok = pl.ds(pl.multiple_of(r * 512, 512), 512)

            @pl.when(valid_ref[r] > 0)
            def _():
                out_ref[tok, :] = (x_ref[tok, :].astype(F32) + u_s[tok, :]).astype(BF16)

            @pl.when(valid_ref[r] == 0)
            def _():
                out_ref[tok, :] = x_ref[tok, :]

            return carry

        lax.fori_loop(0, 8, write, 0)


def attend(x, bg, gain, shift, wp, gb, wo, ob, valid):
    vmem = pl.BlockSpec(memory_space=pltpu.VMEM)
    v = pltpu.VMEM
    return pl.pallas_call(
        attend_kernel,
        out_shape=jax.ShapeDtypeStruct((4096, C), BF16),
        in_specs=[pl.BlockSpec(memory_space=pltpu.SMEM)] + [vmem] * 8,
        out_specs=vmem,
        scratch_shapes=[
            v((JW, 4, H, 256, 256), BF16),
            v((JW, 1024, 256), BF16),
            v((JW, 4, H, 256, 256), BF16),
            v((JW, 1024, C), F32),
            v((512, C), F32), v((512, C), F32), v((512, C), F32), v((512, C), F32),
            v((256, H * 256), BF16),
            v((256, 256), F32),
            v((4096, C), F32),
            v((H, 256, C), F32),
            v((2, 8, C), F32),
            pltpu.SMEM((16,), jnp.int32),
        ],
        compiler_params=pltpu.CompilerParams(vmem_limit_bytes=60 * 1024 * 1024),
        name="attend",
    )(valid, x, bg, gain, shift, wp, gb, wo, ob)


def shards(pair_rep, ln_gain, ln_shift, w_proj, gate_bias, w_bias, w_out, out_bias, block_valid):
    gain, shift = ln_gain[None], ln_shift[None]
    wb = jnp.concatenate([w_bias.T, jnp.zeros((8 - H, C), BF16)], axis=0)
    blk = local_bias(pair_rep, gain, shift, wb)
    columns, bias = exchange(pair_rep, blk)
    y = attend(
        columns.reshape(4096, C), bias, gain, shift, w_proj, gate_bias[None], w_out, out_bias[None],
        block_valid,
    )
    out = send_back(y.reshape(ROWS, BLK, JW, C))
    return out.reshape(BLK, COLS, C)


def solution(mesh):
    return jax.shard_map(
        shards,
        mesh=mesh,
        in_specs=(P("row", "col", None), P(), P(), P(), P(), P(), P(), P(), P()),
        out_specs=P("row", "col", None),
        check_vma=False,
    )
```

```python
import jax
import jax.numpy as jnp
from jax import lax
from jax.experimental import pallas as pl
from jax.experimental.pallas import tpu as pltpu
from jax.sharding import PartitionSpec as P

H = 4
HD = 32
C = 128
ROWS = 8
COLS = 32
BLK = 128
JW = 4
BROWS = H * 32 + 8
COLOR_Z = (0, 64)
COLOR_Y = (64, 96)
COLOR_X = (96, 136)
MESH = pl.DeviceIdType.MESH
F32 = jnp.float32
BF16 = jnp.bfloat16
NEG = -1e30


def dot_nt(a, b):
    return lax.dot_general(a, b, (((1,), (1,)), ((), ())), preferred_element_type=F32)


def dot_nn(a, b):
    return lax.dot_general(a, b, (((1,), (0,)), ((), ())), preferred_element_type=F32)


def layer_norm(x, gain, shift):
    average = jnp.mean(x, axis=-1, keepdims=True)
    centred = x - average
    spread = jnp.mean(centred * centred, axis=-1, keepdims=True)
    return (centred * lax.rsqrt(spread + 1e-05) * gain + shift).astype(BF16)


def bias_kernel(x_ref, gain_ref, shift_ref, wb_ref, blk_ref, n_s, b_s):
    col = lax.axis_index("col")

    def norm(step, carry):
        x = x_ref[pl.ds(step * 16, 16), :, :].astype(F32).reshape(512, C)
        n_s[pl.ds(pl.multiple_of(step * 512, 512), 512), :] = layer_norm(
            x, gain_ref[...], shift_ref[...]
        ).astype(F32)
        return carry

    lax.fori_loop(0, 8, norm, 0)
    lanes = lax.broadcasted_iota(jnp.int32, (8, BLK), 1)
    first = lax.rem(col, 4) * 32
    centres = jnp.zeros((8, BLK), F32)
    for i in range(32):
        rows = n_s[pl.ds(i, BLK, stride=32), :].astype(BF16)
        part = dot_nt(wb_ref[...], rows)
        centre = jnp.max(part, axis=-1, keepdims=True).astype(BF16).astype(F32)
        part = part - centre
        for h in range(H):
            b_s[h * 32 + i : h * 32 + i + 1, :] = part[h : h + 1, :]
        centres = jnp.where(lanes == first + i, centre, centres)
    blk_ref[0 : H * 32, :] = b_s[...].astype(BF16)
    blk_ref[H * 32 :, :] = centres.astype(BF16)


def local_bias(x, gain, shift, wb):
    return pl.pallas_call(
        bias_kernel,
        out_shape=jax.ShapeDtypeStruct((BROWS, BLK), BF16),
        scratch_shapes=[pltpu.VMEM((4096, C), F32), pltpu.VMEM((H * 32, BLK), F32)],
        compiler_params=pltpu.CompilerParams(vmem_limit_bytes=60 * 1024 * 1024),
        name="local_bias",
    )(x, gain, shift, wb)


class Ring:
    def __init__(self, size, mine, unit, at, send, recv):
        self.size, self.mine, self.unit, self.at, self.send, self.recv = size, mine, unit, at, send, recv
        self.last = size // 2

    def copy(self, way, step, place):
        half = way if step == self.last else None
        sign = 1 - 2 * way
        return pltpu.make_async_remote_copy(
            src_ref=self.unit(place, half),
            dst_ref=self.unit(place, half),
            send_sem=self.send.at[way, step - 1],
            recv_sem=self.recv.at[way, step - 1],
            device_id=self.at(lax.rem(self.mine + sign + self.size, self.size)),
            device_id_type=MESH,
        )

    def away(self, way, steps):
        return lax.rem(self.mine - (1 - 2 * way) * steps + self.size, self.size)

    def hop(self, way, step):
        return self.copy(way, step, self.away(way, step - 1))

    def arrival(self, way, step):
        return self.copy(way, step, self.away(way, step))


def exchange_kernel(
    x_ref, blk_ref, o_ref, bg_out,
    bg, stage, a_send, a_recv, f_send, f_recv, pz_send, pz_recv, pq_send, pq_recv,
    r0s, r0r, r1s, r1r, r2s, r2r, r3s, r3r, r4s, r4r, r5s, r5r, r6s, r6r, r7s, r7r,
    dz_send, dz_recv, dy_send, dy_recv, dx_send, dx_recv, cz, cy, cx, own_sem,
):
    row = lax.axis_index("row")
    col = lax.axis_index("col")
    xl, y = row // 4, lax.rem(row, 4)
    z, xh, core = col // 4, lax.rem(col // 2, 2), lax.rem(col, 2)
    x = xh * 2 + xl
    every = slice(None)

    def device(x_, y_, z_, core_=None):
        core_ = core if core_ is None else core_
        return {"row": lax.rem(x_, 2) * 4 + y_, "col": z_ * 4 + (x_ // 2) * 2 + core_}

    rows_z = pl.ds(COLOR_Z[0], COLOR_Z[1] - COLOR_Z[0])
    rows_y = pl.ds(COLOR_Y[0], COLOR_Y[1] - COLOR_Y[0])
    rows_x = pl.ds(COLOR_X[0], COLOR_X[1] - COLOR_X[0])
    rows_q = pl.ds(COLOR_Y[0], COLOR_X[1] - COLOR_Y[0])

    def part(half, count):
        return every if half is None else pl.ds(half * count, count)

    def unit_zx(p, half):
        return bg.at[lax.rem(p, 2), part(half, 2), z, p // 2, core, rows_z, :]

    def unit_yx(p, half):
        return bg.at[lax.rem(p, 2), y, part(half, 4), p // 2, core, rows_y, :]

    def unit_xy(p, half):
        return bg.at[xl, p, part(half, 4), xh, core, rows_x, :]

    def unit_za(p, half):
        return bg.at[xl, part(half, 2), p, xh, core, rows_z, :]

    def unit_zb(p, half):
        return bg.at[1 - xl, part(half, 2), p, :, core, rows_z, :]

    def unit_zc(p, half):
        return bg.at[xl, part(half, 2), p, 1 - xh, core, rows_z, :]

    def unit_z(p, half, ref=bg, core=core):
        return ref.at[part(half, 1), :, p, :, core, rows_z, :]

    def unit_y(p, half, ref=bg, core=core):
        return ref.at[part(half, 1), p, :, :, core, rows_y, :]

    def unit_x(p, half, ref=bg, core=core):
        return ref.at[lax.rem(p, 2), part(half, 2), :, p // 2, core, rows_x, :]

    zx = Ring(4, x, unit_zx, lambda p: device(p, y, z), r0s, r0r)
    yx = Ring(4, x, unit_yx, lambda p: device(p, y, z), r1s, r1r)
    xy = Ring(4, y, unit_xy, lambda p: device(x, p, z), r2s, r2r)
    along_z = lambda p: device(x, y, p)
    za = Ring(8, z, unit_za, along_z, r3s, r3r)
    zb = Ring(8, z, unit_zb, along_z, r6s, r6r)
    zc = Ring(8, z, unit_zc, along_z, r7s, r7r)
    rz = Ring(8, z, unit_z, along_z, None, None)
    ry = Ring(4, y, unit_y, lambda p: device(x, p, z), r4s, r4r)
    rx = Ring(4, x, unit_x, lambda p: device(p, y, z), r5s, r5r)
    finals = ((rz, dz_send, dz_recv, cz), (ry, dy_send, dy_recv, cy), (rx, dx_send, dx_recv, cx))

    def round_line(mine, size, act):
        def body(d, carry):
            act(lax.rem(mine + d, size))
            return carry

        lax.fori_loop(1, size, body, 0)

    barrier = pltpu.get_barrier_semaphore()

    def greet(target):
        pl.semaphore_signal(barrier, inc=1, device_id=target, device_id_type=MESH)

    round_line(z, 8, lambda p: greet(device(x, y, p)))
    round_line(x, 4, lambda p: greet(device(p, y, z)))
    round_line(row, ROWS, lambda p: greet({"row": p, "col": col}))
    greet(device(x, y, z, 1 - core))
    pl.semaphore_wait(barrier, 18)

    def line_z(p, sender):
        return pltpu.make_async_remote_copy(
            src_ref=blk_ref.at[rows_z, :],
            dst_ref=bg.at[xl, sender, z, xh, core, rows_z, :],
            send_sem=pz_send.at[p],
            recv_sem=pz_recv.at[sender],
            device_id=device(x, p, z),
            device_id_type=MESH,
        )

    def line_q(p, sender):
        return pltpu.make_async_remote_copy(
            src_ref=blk_ref.at[rows_q, :],
            dst_ref=bg.at[xl, y, sender, xh, core, rows_q, :],
            send_sem=pq_send.at[p],
            recv_sem=pq_recv.at[sender],
            device_id=device(x, y, p),
            device_id_type=MESH,
        )

    bg[xl, y, z, xh, core] = blk_ref[...]
    round_line(y, 4, lambda p: line_z(p, y).start())
    round_line(z, 8, lambda p: line_q(p, z).start())

    def column(dx, dy, arriving=False):
        sign = -1 if arriving else 1
        px, py = lax.rem(xl + dx, 2), lax.rem(y + sign * dy + 4, 4)
        peer = px * 4 + py
        return pltpu.make_async_remote_copy(
            src_ref=x_ref.at[:, peer],
            dst_ref=o_ref.at[peer if arriving else row],
            send_sem=a_send.at[dx * 4 + dy],
            recv_sem=a_recv.at[dx * 4 + dy],
            device_id={"row": peer, "col": col},
            device_id_type=MESH,
        )

    def corner_out():
        return pltpu.make_async_remote_copy(
            src_ref=x_ref.at[:, (1 - xl) * 4 + lax.rem(y + 2, 4)],
            dst_ref=stage,
            send_sem=f_send.at[0],
            recv_sem=f_recv.at[0],
            device_id={"row": xl * 4 + lax.rem(y + 3, 4), "col": col},
            device_id_type=MESH,
        )

    def corner_on():
        return pltpu.make_async_remote_copy(
            src_ref=stage,
            dst_ref=o_ref.at[xl * 4 + lax.rem(y + 1, 4)],
            send_sem=f_send.at[1],
            recv_sem=f_recv.at[1],
            device_id={"row": (1 - xl) * 4 + lax.rem(y + 3, 4), "col": col},
            device_id_type=MESH,
        )

    def corner_in():
        return pltpu.make_async_remote_copy(
            src_ref=stage,
            dst_ref=o_ref.at[(1 - xl) * 4 + lax.rem(y + 2, 4)],
            send_sem=f_send.at[1],
            recv_sem=f_recv.at[1],
            device_id={"row": (1 - xl) * 4 + lax.rem(y + 3, 4), "col": col},
            device_id_type=MESH,
        )

    keep = pltpu.make_async_copy(x_ref.at[:, row], o_ref.at[row], own_sem.at[0])
    keep.start()
    early = ((1, 0), (0, 1), (0, 3))
    late = ((1, 1), (1, 3), (0, 2))
    for dx, dy in early:
        column(dx, dy).start()

    def launch(ring, step):
        for way in (0, 1):
            ring.hop(way, step).start()

    def await_step(ring, step):
        for way in (0, 1):
            ring.arrival(way, step).wait_recv()

    def across(final, place):
        ring, send, recv, _ = final
        return pltpu.make_async_remote_copy(
            src_ref=ring.unit(place, None),
            dst_ref=ring.unit(place, None),
            send_sem=send.at[place],
            recv_sem=recv.at[place],
            device_id=device(x, y, z, 1 - core),
            device_id_type=MESH,
        )

    def across_arrival(final, place):
        ring, send, recv, _ = final
        other = ring.unit(place, None, bg, 1 - core)
        return pltpu.make_async_remote_copy(
            src_ref=other, dst_ref=other, send_sem=send.at[place], recv_sem=recv.at[place],
            device_id=device(x, y, z, 1 - core), device_id_type=MESH,
        )

    def keep_unit(final, place, which):
        ring, _, _, sem = final
        side = core if which == 0 else 1 - core
        return pltpu.make_async_copy(
            ring.unit(place, None, bg, side), ring.unit(place, None, bg_out, side), sem.at[which, place]
        )

    def hand_on(final, place):
        across(final, place).start()
        keep_unit(final, place, 0).start()

    def onward(ring, step):
        for way in (0, 1):
            ring.arrival(way, step).wait_recv()
            if step < ring.last:
                ring.hop(way, step + 1).start()

    def advance(final, step):
        ring = final[0]
        for way in (0, 1):
            ring.arrival(way, step).wait_recv()
            if step < ring.last:
                ring.hop(way, step + 1).start()
                hand_on(final, ring.away(way, step))
        if step == ring.last:
            hand_on(final, ring.away(0, step))

    def hand_z(step):
        hand_on(finals[0], rz.away(0, step))
        if step < 4:
            hand_on(finals[0], rz.away(1, step))

    round_line(y, 4, lambda p: line_z(p, p).wait_recv())
    launch(za, 1)
    launch(zx, 1)
    await_step(zx, 1)
    launch(zb, 1)
    launch(zx, 2)
    round_line(z, 8, lambda p: line_q(p, p).wait_recv())
    launch(yx, 1)
    launch(xy, 1)
    onward(za, 1)
    await_step(zx, 2)
    launch(zc, 1)
    hand_on(finals[0], z)
    await_step(xy, 1)
    launch(xy, 2)
    await_step(yx, 1)
    launch(yx, 2)
    corner_out().start()
    onward(zb, 1)
    await_step(xy, 2)
    launch(rx, 1)
    hand_on(finals[2], x)
    await_step(yx, 2)
    launch(ry, 1)
    hand_on(finals[1], y)
    onward(za, 2)
    onward(zc, 1)
    hand_z(1)
    for dx, dy in late:
        column(dx, dy).start()
    corner_out().wait_recv()
    corner_on().start()
    onward(zb, 2)
    onward(za, 3)
    onward(zc, 2)
    hand_z(2)
    advance(finals[2], 1)
    advance(finals[1], 1)
    onward(zb, 3)
    onward(za, 4)
    onward(zc, 3)
    hand_z(3)
    advance(finals[2], 2)
    advance(finals[1], 2)
    onward(zb, 4)
    onward(zc, 4)
    hand_z(4)

    for final in (finals[1], finals[2], finals[0]):
        ring = final[0]
        for d in range(ring.size):
            place = ring.away(d % 2, (d + 1) // 2)
            across_arrival(final, place).wait_recv()
            keep_unit(final, place, 1).start()
    round_line(y, 4, lambda p: line_z(p, y).wait_send())
    round_line(z, 8, lambda p: line_q(p, z).wait_send())
    for ring in (zx, yx, xy, za, zb, zc, ry, rx):
        for way in (0, 1):
            for step in range(1, ring.last + 1):
                ring.hop(way, step).wait_send()
    for dx, dy in early + late:
        column(dx, dy).wait_send()
        column(dx, dy, True).wait_recv()
    corner_out().wait_send()
    corner_on().wait_send()
    corner_in().wait_recv()
    keep.wait()
    for final in finals:
        for place in range(final[0].size):
            across(final, place).wait_send()
            keep_unit(final, place, 0).wait()
            keep_unit(final, place, 1).wait()


def exchange(x, blk):
    dma = pltpu.SemaphoreType.DMA
    sems = [dma((8,)), dma((8,)), dma((2,)), dma((2,)), dma((4,)), dma((4,)), dma((8,)), dma((8,))]
    for size in (2, 2, 2, 4, 2, 2, 4, 4):
        sems += [dma((2, size)), dma((2, size))]
    sems += [dma((8,)), dma((8,)), dma((4,)), dma((4,)), dma((4,)), dma((4,))]
    sems += [dma((2, 8)), dma((2, 4)), dma((2, 4)), dma((1,))]
    shape = (2, 4, 8, 2, 2, BROWS, BLK)
    hbm = pl.BlockSpec(memory_space=pl.ANY)
    return pl.pallas_call(
        exchange_kernel,
        out_shape=(
            jax.ShapeDtypeStruct((ROWS, BLK, JW, C), BF16),
            jax.ShapeDtypeStruct(shape, BF16),
        ),
        in_specs=[hbm, pl.BlockSpec(memory_space=pltpu.VMEM)],
        out_specs=(hbm, hbm),
        scratch_shapes=[pltpu.VMEM(shape, BF16), pltpu.VMEM((BLK, JW, C), BF16)] + sems,
        compiler_params=pltpu.CompilerParams(
            collective_id=0, has_side_effects=True, vmem_limit_bytes=48 * 1024 * 1024
        ),
        name="exchange",
    )(x.reshape(BLK, ROWS, JW, C), blk)


def return_kernel(y_ref, o_ref, send, recv, local_sem):
    row = lax.axis_index("row")
    barrier = pltpu.get_barrier_semaphore()
    for d in range(1, ROWS):
        pl.semaphore_signal(
            barrier, inc=1, device_id={"row": lax.rem(row + d, ROWS)}, device_id_type=MESH
        )
    pl.semaphore_wait(barrier, ROWS - 1)

    def copy(peer, sender):
        return pltpu.make_async_remote_copy(
            src_ref=y_ref.at[peer],
            dst_ref=o_ref.at[:, sender],
            send_sem=send.at[peer],
            recv_sem=recv.at[sender],
            device_id={"row": peer},
            device_id_type=MESH,
        )

    for d in range(1, ROWS):
        copy(lax.rem(row + d, ROWS), row).start()
    keep = pltpu.make_async_copy(y_ref.at[row], o_ref.at[:, row], local_sem)
    keep.start()
    for d in range(1, ROWS):
        peer = lax.rem(row + d, ROWS)
        copy(peer, row).wait_send()
        copy(peer, peer).wait_recv()
    keep.wait()


def send_back(y):
    dma = pltpu.SemaphoreType.DMA
    return pl.pallas_call(
        return_kernel,
        out_shape=jax.ShapeDtypeStruct((BLK, ROWS, JW, C), BF16),
        in_specs=[pl.BlockSpec(memory_space=pl.ANY)],
        out_specs=pl.BlockSpec(memory_space=pl.ANY),
        scratch_shapes=[dma((8,)), dma((8,)), dma],
        compiler_params=pltpu.CompilerParams(collective_id=1, has_side_effects=True),
        name="send_back",
    )(y)


def attend_kernel(
    valid_ref, x_ref, bg_ref, gain_ref, shift_ref, wp_ref, gb_ref, wo_ref, ob_ref, out_ref,
    bgv, q_s, e_s, k_s, kp_s, v_s, one_s, g_s, tq, tk, tv, tg, p0, p1, p2, p3, acc0, acc1, acc2, acc3, u_s, mx_s, top_s,
    idx_s, bias_sem,
):
    ps, accs = (p0, p1, p2, p3), (acc0, acc1, acc2, acc3)
    col = lax.axis_index("col")
    present = valid_ref[col // 4]

    def place(b, count):
        idx_s[count] = b
        return count + valid_ref[b]

    n = lax.fori_loop(0, 8, place, 0)
    idx_s[n] = 0
    pairs = (n + 1) // 2
    lanes = lax.broadcasted_iota(jnp.int32, (BLK, C), 1)

    def bias_copy(step):
        sk, si = step // n, lax.rem(step, n)
        rk, ri = idx_s[sk], idx_s[si]
        return pltpu.make_async_copy(
            bg_ref.at[rk // 4, lax.rem(rk, 4), ri], bgv.at[sk, si], bias_sem.at[sk * 8 + si]
        )

    @pl.when(present == 0)
    def _():
        out_ref[...] = x_ref[...]

    @pl.when(present != 0)
    def _():
        def fetch(step, carry):
            bias_copy(step).start()
            return carry

        lax.fori_loop(0, n * n, fetch, 0)
        top_s[...] = jnp.zeros_like(top_s)
        for h in range(H):
            one_s[h * 256 : (h + 1) * 256, :] = jnp.where(
                lax.broadcasted_iota(jnp.int32, (256, C), 1) // HD == h, 1.0, 0.0
            ).astype(BF16)

        def prepare(s, carry):
            r = idx_s[s]
            tok = pl.multiple_of(r * 512, 512)
            x = x_ref[pl.ds(tok, 512), :].astype(F32)
            normed = layer_norm(x, gain_ref[...], shift_ref[...])
            proj = dot_nn(normed, wp_ref[...])
            q = (proj[:, :C] * (HD ** -0.5)).astype(BF16)
            k = proj[:, C : 2 * C].astype(BF16)
            tq[...] = q.astype(F32)
            tk[...] = k.astype(F32)
            tv[...] = proj[:, 2 * C : 3 * C]
            tg[...] = jax.nn.sigmoid(proj[:, 3 * C :] + gb_ref[...])
            heads = (
                lax.broadcasted_iota(jnp.int32, (C, C), 0) // HD
                == lax.broadcasted_iota(jnp.int32, (C, C), 1) // HD
            ).astype(BF16)
            q2 = dot_nn(q * q, heads)
            k2 = dot_nn(k * k, heads)
            top_s[0] = jnp.maximum(top_s[0], jnp.max(q2.reshape(64, 8, C), axis=0))
            top_s[1] = jnp.maximum(top_s[1], jnp.max(k2.reshape(64, 8, C), axis=0))
            at = pl.multiple_of(s * BLK, BLK)
            it = s // 2
            sub = pl.multiple_of(lax.rem(s, 2) * BLK, BLK)
            for j in range(JW):
                qj = tq[pl.ds(j, BLK, stride=JW), :].astype(BF16)
                vj = tv[pl.ds(j, BLK, stride=JW), :].astype(BF16)
                k_s[j, pl.ds(at, BLK), :] = tk[pl.ds(j, BLK, stride=JW), :].astype(BF16)
                g_s[j, pl.ds(at, BLK), :] = tg[pl.ds(j, BLK, stride=JW), :]
                for h in range(H):
                    pick = one_s[h * 256 : h * 256 + BLK, :]
                    q_s[j, it, h, pl.ds(sub, BLK), :] = qj * pick
                    v_s[j, it, pl.ds(h * 256 + sub, BLK), :] = vj * pick
            kp_s[pl.ds(at, BLK), :] = jnp.where(
                (lanes // 8 == s) | (lanes // 8 == 8), 1.0, 0.0
            ).astype(BF16)
            return carry

        lax.fori_loop(0, n, prepare, 0)

        def fetched(step, carry):
            bias_copy(step).wait()
            return carry

        lax.fori_loop(0, n * n, fetched, 0)

        def centre(s, carry):
            tiles = []
            high = jnp.full((8, BLK), NEG, F32)
            for b in range(8):
                part = bgv[b, s, 0, 0, H * 32 :, :].astype(F32)
                for q4 in range(1, 4):
                    part = part + bgv[b, s, q4 // 2, q4 % 2, H * 32 :, :].astype(F32)
                tiles.append(jnp.where(b < n, part, 0.0))
                high = jnp.maximum(high, jnp.where(b < n, part, NEG))
            tiles.append(-high)
            tiles.append(jnp.full((8, BLK), NEG, F32))
            tiles.append(jnp.zeros((48, BLK), F32))
            turned = jnp.concatenate(tiles, axis=0).T
            it = s // 2
            sub = pl.multiple_of(lax.rem(s, 2) * BLK, BLK)
            for h in range(H):
                e_s[it, h, pl.ds(sub, BLK), :] = jnp.where(
                    ((lax.rem(lanes, 8) == h) & (lanes < 72)) | (lanes == 72), turned, 0.0
                ).astype(BF16)
            return carry

        lax.fori_loop(0, n, centre, 0)

        @pl.when(lax.rem(n, 2) == 1)
        def _():
            at = pl.multiple_of(n * BLK, BLK)
            it = n // 2
            zero = jnp.zeros((BLK, C), BF16)
            kp_s[pl.ds(at, BLK), :] = jnp.where(lanes == 72, 1.0, 0.0).astype(BF16)
            for j in range(JW):
                k_s[j, pl.ds(at, BLK), :] = zero
                for h in range(H):
                    v_s[j, it, h * 256 + BLK : h * 256 + 256, :] = zero
                    q_s[j, it, h, BLK : 2 * BLK, :] = zero
            for h in range(H):
                e_s[it, h, BLK : 2 * BLK, :] = zero

        bound = jnp.max(jnp.max(top_s[0], axis=0, keepdims=True) * jnp.max(top_s[1], axis=0, keepdims=True))

        def scores(j, it, kt, h):
            keys = pl.ds(pl.multiple_of(kt * 256, 256), 256)
            s = dot_nt(
                jnp.concatenate([q_s[j, it, h], e_s[it, h]], axis=1),
                jnp.concatenate([k_s[j, keys, :], kp_s[keys, :]], axis=1),
            )
            rows = []
            for a in range(2):
                si = jnp.minimum(it * 2 + a, n - 1)
                parts = []
                for b in range(2):
                    sk = jnp.minimum(kt * 2 + b, n - 1)
                    bias = bgv[sk, si, :, :, h * 32 : h * 32 + 32, :]
                    parts.append(
                        s[a * BLK : (a + 1) * BLK, b * BLK : (b + 1) * BLK]
                        + bias.reshape(BLK, BLK).astype(F32)
                    )
                rows.append(jnp.concatenate(parts, axis=1))
            return jnp.concatenate(rows, axis=0)

        def weigh(p_ref, j, it, kt, shifted):
            for h in range(H):
                s = scores(j, it, kt, h)
                if shifted:
                    s = s - mx_s[h][:, 0:1]
                p_ref[:, h * 256 : (h + 1) * 256] = jnp.exp(s).astype(BF16)

        def gather_values(p_ref, j, kt, to_ref, from_ref):
            got = dot_nn(p_ref[...], jnp.concatenate([v_s[j, kt], one_s[...]], axis=1))
            to_ref[...] = jnp.where(kt == 0, 0.0, from_ref[...]) + got

        def finish(j, it, acc):
            base = pl.multiple_of(it * 256, 256)
            mixed = (acc[:, 0:C] / acc[:, C : 2 * C]).astype(BF16).astype(F32)
            gated = (g_s[j, pl.ds(base, 256), :] * mixed).astype(BF16)
            update = dot_nn(gated, wo_ref[...]) + ob_ref[...]
            for a in range(2):
                ri = idx_s[it * 2 + a]

                @pl.when(it * 2 + a < n)
                def _():
                    u_s[pl.ds(ri * 512 + j, BLK, stride=JW), :] = update[a * BLK : (a + 1) * BLK]

        def four_columns(step, carry):
            it, kt = step // pairs, lax.rem(step, pairs)
            before = jnp.maximum(step - 1, 0)
            it0, kt0 = before // pairs, lax.rem(before, pairs)
            weigh(ps[0], 0, it, kt, False)
            gather_values(ps[3], 3, kt0, accs[3], accs[3])
            for j in range(1, JW):
                weigh(ps[j], j, it, kt, False)
                gather_values(ps[j - 1], j - 1, kt, accs[j - 1], accs[j - 1])

            @pl.when((kt0 == pairs - 1) & (step > 0))
            def _():
                finish(3, it0, accs[3])

            @pl.when(kt == pairs - 1)
            def _():
                for j in range(3):
                    finish(j, it, accs[j])

            return carry

        def over_tiles_shifted(step, carry):
            j, it = step // pairs, lax.rem(step, pairs)
            mx_s[...] = jnp.full_like(mx_s, NEG)

            def highest(kt, inner):
                for h in range(H):
                    top = jnp.max(scores(j, it, kt, h), axis=-1, keepdims=True)
                    mx_s[h] = jnp.maximum(mx_s[h], top)
                return inner

            def sum_up(kt, inner):
                weigh(p0, j, it, kt, True)
                gather_values(p0, j, kt, acc0, acc0)
                return inner

            lax.fori_loop(0, pairs, highest, 0)
            lax.fori_loop(0, pairs, sum_up, 0)
            finish(j, it, acc0)
            return carry

        @pl.when(bound <= 3000.0)
        def _():
            lax.fori_loop(0, pairs * pairs, four_columns, 0)
            gather_values(ps[3], 3, pairs - 1, accs[3], accs[3])
            finish(3, pairs - 1, accs[3])

        @pl.when(jnp.logical_not(bound <= 3000.0))
        def _():
            lax.fori_loop(0, pairs * JW, over_tiles_shifted, 0)

        def write(r, carry):
            tok = pl.ds(pl.multiple_of(r * 512, 512), 512)

            @pl.when(valid_ref[r] > 0)
            def _():
                out_ref[tok, :] = (x_ref[tok, :].astype(F32) + u_s[tok, :]).astype(BF16)

            @pl.when(valid_ref[r] == 0)
            def _():
                out_ref[tok, :] = x_ref[tok, :]

            return carry

        lax.fori_loop(0, 8, write, 0)


def attend(x, bg, gain, shift, wp, gb, wo, ob, valid):
    vmem = pl.BlockSpec(memory_space=pltpu.VMEM)
    v = pltpu.VMEM
    return pl.pallas_call(
        attend_kernel,
        out_shape=jax.ShapeDtypeStruct((4096, C), BF16),
        in_specs=[pl.BlockSpec(memory_space=pltpu.SMEM), vmem, pl.BlockSpec(memory_space=pl.ANY)]
        + [vmem] * 6,
        out_specs=vmem,
        scratch_shapes=[
            v((8, 8, 2, 2, BROWS, BLK), BF16),
            v((JW, 4, H, 256, C), BF16),
            v((4, H, 256, C), BF16),
            v((JW, 1024, C), BF16),
            v((1024, C), BF16),
            v((JW, 4, H * 256, C), BF16),
            v((H * 256, C), BF16),
            v((JW, 1024, C), F32),
            v((512, C), F32), v((512, C), F32), v((512, C), F32), v((512, C), F32),
            v((256, H * 256), BF16), v((256, H * 256), BF16), v((256, H * 256), BF16), v((256, H * 256), BF16),
            v((256, 256), F32), v((256, 256), F32), v((256, 256), F32), v((256, 256), F32),
            v((4096, C), F32),
            v((H, 256, C), F32),
            v((2, 8, C), F32),
            pltpu.SMEM((16,), jnp.int32),
            pltpu.SemaphoreType.DMA((64,)),
        ],
        compiler_params=pltpu.CompilerParams(vmem_limit_bytes=60 * 1024 * 1024),
        name="attend",
    )(valid, x, bg, gain, shift, wp, gb, wo, ob)


def shards(pair_rep, ln_gain, ln_shift, w_proj, gate_bias, w_bias, w_out, out_bias, block_valid):
    gain, shift = ln_gain[None], ln_shift[None]
    wb = jnp.concatenate([w_bias.T, jnp.zeros((8 - H, C), BF16)], axis=0)
    blk = local_bias(pair_rep, gain, shift, wb)
    columns, bias = exchange(pair_rep, blk)
    y = attend(
        columns.reshape(4096, C), bias, gain, shift, w_proj, gate_bias[None], w_out, out_bias[None],
        block_valid,
    )
    out = send_back(y.reshape(ROWS, BLK, JW, C))
    return out.reshape(BLK, COLS, C)


def solution(mesh):
    return jax.shard_map(
        shards,
        mesh=mesh,
        in_specs=(P("row", "col", None), P(), P(), P(), P(), P(), P(), P(), P()),
        out_specs=P("row", "col", None),
        check_vma=False,
    )
```

```python
import jax
import jax.numpy as jnp
from jax import lax
from jax.experimental import pallas as pl
from jax.experimental.pallas import tpu as pltpu
from jax.sharding import PartitionSpec as P

H = 4
HD = 32
C = 128
ROWS = 8
COLS = 32
BLK = 128
JW = 4
BROWS = H * 32 + 8
COLOR_Z = (0, 64)
COLOR_Y = (64, 96)
COLOR_X = (96, 136)
MESH = pl.DeviceIdType.MESH
F32 = jnp.float32
BF16 = jnp.bfloat16
NEG = -1e30


def dot_nt(a, b):
    return lax.dot_general(a, b, (((1,), (1,)), ((), ())), preferred_element_type=F32)


def dot_nn(a, b):
    return lax.dot_general(a, b, (((1,), (0,)), ((), ())), preferred_element_type=F32)


def layer_norm(x, gain, shift):
    average = jnp.mean(x, axis=-1, keepdims=True)
    centred = x - average
    spread = jnp.mean(centred * centred, axis=-1, keepdims=True)
    return (centred * lax.rsqrt(spread + 1e-05) * gain + shift).astype(BF16)


def normalise_block(xv, gain_ref, shift_ref, n_s):
    def norm(step, carry):
        x = xv[pl.ds(step * 16, 16), :, :].astype(F32).reshape(512, C)
        n_s[pl.ds(pl.multiple_of(step * 512, 512), 512), :] = layer_norm(
            x, gain_ref[...], shift_ref[...]
        ).astype(F32)
        return carry

    lax.fori_loop(0, 8, norm, 0)


def bias_block(wb_ref, n_s, b_s, blk_ref, col):
    wide = wb_ref[...].astype(F32)
    wide = jnp.concatenate([wide, jnp.zeros((8 - H, C), F32)], axis=0).astype(BF16)
    lanes = lax.broadcasted_iota(jnp.int32, (8, BLK), 1)
    first = lax.rem(col, 4) * 32
    centres = jnp.zeros((8, BLK), F32)
    for i in range(32):
        part = dot_nt(wide, n_s[pl.ds(i, BLK, stride=32), :].astype(BF16))
        centre = jnp.max(part, axis=-1, keepdims=True).astype(BF16).astype(F32)
        part = part - centre
        for h in range(H):
            b_s[h * 32 + i : h * 32 + i + 1, :] = part[h : h + 1, :]
        centres = jnp.where(lanes == first + i, centre, centres)
    blk_ref[0 : H * 32, :] = b_s[...].astype(BF16)
    blk_ref[H * 32 :, :] = centres.astype(BF16)


class Ring:
    def __init__(self, size, mine, unit, at, send, recv):
        self.size, self.mine, self.unit, self.at, self.send, self.recv = size, mine, unit, at, send, recv
        self.last = size // 2

    def copy(self, way, step, place):
        half = way if step == self.last else None
        sign = 1 - 2 * way
        return pltpu.make_async_remote_copy(
            src_ref=self.unit(place, half),
            dst_ref=self.unit(place, half),
            send_sem=self.send.at[way, step - 1],
            recv_sem=self.recv.at[way, step - 1],
            device_id=self.at(lax.rem(self.mine + sign + self.size, self.size)),
            device_id_type=MESH,
        )

    def away(self, way, steps):
        return lax.rem(self.mine - (1 - 2 * way) * steps + self.size, self.size)

    def hop(self, way, step):
        return self.copy(way, step, self.away(way, step - 1))

    def arrival(self, way, step):
        return self.copy(way, step, self.away(way, step))


def exchange_kernel(
    x_ref, flat_ref, gain_ref, shift_ref, wb_ref, o_ref, bg_out,
    bg, xv, n_s, b_s, blk_ref, a_send, a_recv, pz_send, pz_recv, pq_send, pq_recv,
    r0s, r0r, r1s, r1r, r2s, r2r, r3s, r3r, r4s, r4r, r5s, r5r, r6s, r6r, r7s, r7r,
    r8s, r8r, r9s, r9r, ras, rar, rbs, rbr,
    dz_send, dz_recv, dy_send, dy_recv, dx_send, dx_recv, cz, cy, cx, own_sem,
):
    row = lax.axis_index("row")
    col = lax.axis_index("col")
    xl, y = row // 4, lax.rem(row, 4)
    z, xh, core = col // 4, lax.rem(col // 2, 2), lax.rem(col, 2)
    x = xh * 2 + xl
    every = slice(None)
    block_in = pltpu.make_async_copy(flat_ref, xv, own_sem.at[1])
    block_in.start()

    def device(x_, y_, z_, core_=None):
        core_ = core if core_ is None else core_
        return {"row": lax.rem(x_, 2) * 4 + y_, "col": z_ * 4 + (x_ // 2) * 2 + core_}

    rows_z = pl.ds(COLOR_Z[0], COLOR_Z[1] - COLOR_Z[0])
    rows_y = pl.ds(COLOR_Y[0], COLOR_Y[1] - COLOR_Y[0])
    rows_x = pl.ds(COLOR_X[0], COLOR_X[1] - COLOR_X[0])
    rows_q = pl.ds(COLOR_Y[0], COLOR_X[1] - COLOR_Y[0])

    def part(half, count):
        return every if half is None else pl.ds(half * count, count)

    yh, yl = y // 2, lax.rem(y, 2)

    def unit_zx(p, half):
        return bg.at[lax.rem(p, 2), part(half, 1), :, z, p // 2, core, rows_z, :]

    def unit_yx(p, half):
        return bg.at[lax.rem(p, 2), yh, yl, part(half, 4), p // 2, core, rows_y, :]

    def unit_xy(p, half):
        return bg.at[xl, p // 2, lax.rem(p, 2), part(half, 4), xh, core, rows_x, :]

    def unit_za(p, half):
        return bg.at[xl, part(half, 1), :, p, xh, core, rows_z, :]

    def unit_zb(p, half):
        return bg.at[1 - xl, part(half, 1), :, p, :, core, rows_z, :]

    def unit_zc(p, half):
        return bg.at[xl, part(half, 1), :, p, 1 - xh, core, rows_z, :]

    def unit_ya(p, half):
        return bg.at[xl, p // 2, lax.rem(p, 2), part(half, 4), xh, core, rows_y, :]

    def unit_yb(p, half):
        return bg.at[1 - xl, p // 2, lax.rem(p, 2), part(half, 4), :, core, rows_y, :]

    def unit_yc(p, half):
        return bg.at[xl, p // 2, lax.rem(p, 2), part(half, 4), 1 - xh, core, rows_y, :]

    def unit_xa(p, half):
        return bg.at[lax.rem(p, 2), yh, yl, part(half, 4), p // 2, core, rows_x, :]

    def unit_xb(p, half):
        return bg.at[lax.rem(p, 2), :, 1 - yl, part(half, 4), p // 2, core, rows_x, :]

    def unit_xc(p, half):
        return bg.at[lax.rem(p, 2), 1 - yh, yl, part(half, 4), p // 2, core, rows_x, :]

    def unit_z(p, half, ref=bg, core=core):
        return ref.at[:, :, :, p, :, core, rows_z, :]

    def unit_y(p, half, ref=bg, core=core):
        return ref.at[:, p // 2, lax.rem(p, 2), :, :, core, rows_y, :]

    def unit_x(p, half, ref=bg, core=core):
        return ref.at[lax.rem(p, 2), :, :, :, p // 2, core, rows_x, :]

    along_x = lambda p: device(p, y, z)
    along_y = lambda p: device(x, p, z)
    along_z = lambda p: device(x, y, p)
    zx = Ring(4, x, unit_zx, along_x, r0s, r0r)
    yx = Ring(4, x, unit_yx, along_x, r1s, r1r)
    xy = Ring(4, y, unit_xy, along_y, r2s, r2r)
    za = Ring(8, z, unit_za, along_z, r3s, r3r)
    zb = Ring(8, z, unit_zb, along_z, r6s, r6r)
    zc = Ring(8, z, unit_zc, along_z, r7s, r7r)
    ya = Ring(4, y, unit_ya, along_y, r4s, r4r)
    yb = Ring(4, y, unit_yb, along_y, r8s, r8r)
    yc = Ring(4, y, unit_yc, along_y, r9s, r9r)
    xa = Ring(4, x, unit_xa, along_x, r5s, r5r)
    xb = Ring(4, x, unit_xb, along_x, ras, rar)
    xc = Ring(4, x, unit_xc, along_x, rbs, rbr)
    rz = Ring(8, z, unit_z, along_z, None, None)
    ry = Ring(4, y, unit_y, along_y, None, None)
    rx = Ring(4, x, unit_x, along_x, None, None)
    finals = ((rz, dz_send, dz_recv, cz), (ry, dy_send, dy_recv, cy), (rx, dx_send, dx_recv, cx))

    def round_line(mine, size, act):
        def body(d, carry):
            act(lax.rem(mine + d, size))
            return carry

        lax.fori_loop(1, size, body, 0)

    barrier = pltpu.get_barrier_semaphore()

    def greet(target):
        pl.semaphore_signal(barrier, inc=1, device_id=target, device_id_type=MESH)

    round_line(z, 8, lambda p: greet(device(x, y, p)))
    round_line(x, 4, lambda p: greet(device(p, y, z)))
    round_line(row, ROWS, lambda p: greet({"row": p, "col": col}))
    greet(device(x, y, z, 1 - core))
    block_in.wait()
    normalise_block(xv, gain_ref, shift_ref, n_s)
    pl.semaphore_wait(barrier, 18)

    def line_z(p, sender):
        return pltpu.make_async_remote_copy(
            src_ref=blk_ref.at[rows_z, :],
            dst_ref=bg.at[xl, sender // 2, lax.rem(sender, 2), z, xh, core, rows_z, :],
            send_sem=pz_send.at[p],
            recv_sem=pz_recv.at[sender],
            device_id=device(x, p, z),
            device_id_type=MESH,
        )

    def line_q(p, sender):
        return pltpu.make_async_remote_copy(
            src_ref=blk_ref.at[rows_q, :],
            dst_ref=bg.at[xl, yh, yl, sender, xh, core, rows_q, :],
            send_sem=pq_send.at[p],
            recv_sem=pq_recv.at[sender],
            device_id=device(x, y, p),
            device_id_type=MESH,
        )


    def column(dx, dy, arriving=False):
        sign = -1 if arriving else 1
        px, py = lax.rem(xl + dx, 2), lax.rem(y + sign * dy + 4, 4)
        peer = px * 4 + py
        return pltpu.make_async_remote_copy(
            src_ref=x_ref.at[:, peer],
            dst_ref=o_ref.at[peer if arriving else row],
            send_sem=a_send.at[dx * 4 + dy],
            recv_sem=a_recv.at[dx * 4 + dy],
            device_id={"row": peer, "col": col},
            device_id_type=MESH,
        )

    keep = pltpu.make_async_copy(x_ref.at[:, row], o_ref.at[row], own_sem.at[0])
    keep.start()
    early = ((1, 0), (0, 1), (0, 3), (1, 1))
    late = ((1, 3), (0, 2), (1, 2))
    for dx, dy in early:
        column(dx, dy).start()
    bias_block(wb_ref, n_s, b_s, blk_ref, col)
    bg[xl, yh, yl, z, xh, core] = blk_ref[...]
    round_line(y, 4, lambda p: line_z(p, y).start())
    round_line(z, 8, lambda p: line_q(p, z).start())

    def launch(ring, step):
        for way in (0, 1):
            ring.hop(way, step).start()

    def await_step(ring, step):
        for way in (0, 1):
            ring.arrival(way, step).wait_recv()

    def across(final, place):
        ring, send, recv, _ = final
        return pltpu.make_async_remote_copy(
            src_ref=ring.unit(place, None),
            dst_ref=ring.unit(place, None),
            send_sem=send.at[place],
            recv_sem=recv.at[place],
            device_id=device(x, y, z, 1 - core),
            device_id_type=MESH,
        )

    def across_arrival(final, place):
        ring, send, recv, _ = final
        other = ring.unit(place, None, bg, 1 - core)
        return pltpu.make_async_remote_copy(
            src_ref=other, dst_ref=other, send_sem=send.at[place], recv_sem=recv.at[place],
            device_id=device(x, y, z, 1 - core), device_id_type=MESH,
        )

    def keep_unit(final, place, which):
        ring, _, _, sem = final
        side = core if which == 0 else 1 - core
        return pltpu.make_async_copy(
            ring.unit(place, None, bg, side), ring.unit(place, None, bg_out, side), sem.at[which, place]
        )

    def hand_on(final, place):
        across(final, place).start()
        keep_unit(final, place, 0).start()

    def onward(ring, step):
        for way in (0, 1):
            ring.arrival(way, step).wait_recv()
            if step < ring.last:
                ring.hop(way, step + 1).start()

    def hand_unit(which, step):
        ring = finals[which][0]
        hand_on(finals[which], ring.away(0, step))
        if step < ring.last:
            hand_on(finals[which], ring.away(1, step))

    round_line(y, 4, lambda p: line_z(p, p).wait_recv())
    launch(zx, 1)
    launch(za, 1)
    column(*late[0]).start()
    await_step(zx, 1)
    launch(zx, 2)
    launch(zb, 1)
    round_line(z, 8, lambda p: line_q(p, p).wait_recv())
    launch(yx, 1)
    launch(xy, 1)
    launch(xa, 1)
    launch(ya, 1)
    onward(za, 1)
    column(*late[1]).start()
    await_step(zx, 2)
    launch(zc, 1)
    hand_on(finals[0], z)
    await_step(xy, 1)
    launch(xy, 2)
    launch(xb, 1)
    await_step(yx, 1)
    launch(yx, 2)
    launch(yb, 1)
    column(*late[2]).start()
    onward(zb, 1)
    await_step(xy, 2)
    launch(xc, 1)
    hand_on(finals[2], x)
    await_step(yx, 2)
    launch(yc, 1)
    hand_on(finals[1], y)
    onward(xa, 1)
    onward(ya, 1)
    onward(za, 2)
    onward(zc, 1)
    hand_unit(0, 1)
    onward(xb, 1)
    onward(yb, 1)
    onward(zb, 2)
    onward(xc, 1)
    hand_unit(2, 1)
    onward(yc, 1)
    hand_unit(1, 1)
    onward(za, 3)
    onward(zc, 2)
    hand_unit(0, 2)
    onward(xa, 2)
    onward(xb, 2)
    onward(xc, 2)
    hand_unit(2, 2)
    onward(ya, 2)
    onward(yb, 2)
    onward(yc, 2)
    hand_unit(1, 2)
    onward(zb, 3)
    onward(za, 4)
    onward(zc, 3)
    hand_unit(0, 3)
    onward(zb, 4)
    onward(zc, 4)
    hand_unit(0, 4)

    for final in (finals[1], finals[2], finals[0]):
        ring = final[0]
        for d in range(ring.size):
            place = ring.away(d % 2, (d + 1) // 2)
            across_arrival(final, place).wait_recv()
            keep_unit(final, place, 1).start()
    round_line(y, 4, lambda p: line_z(p, y).wait_send())
    round_line(z, 8, lambda p: line_q(p, z).wait_send())
    for ring in (zx, yx, xy, za, zb, zc, ya, yb, yc, xa, xb, xc):
        for way in (0, 1):
            for step in range(1, ring.last + 1):
                ring.hop(way, step).wait_send()
    for dx, dy in early + late:
        column(dx, dy).wait_send()
        column(dx, dy, True).wait_recv()
    keep.wait()
    for final in finals:
        for place in range(final[0].size):
            across(final, place).wait_send()
            keep_unit(final, place, 0).wait()
            keep_unit(final, place, 1).wait()


def exchange(x, gain, shift, wb):
    dma = pltpu.SemaphoreType.DMA
    sems = [dma((8,)), dma((8,)), dma((4,)), dma((4,)), dma((8,)), dma((8,))]
    for size in (2, 2, 2, 4, 2, 2, 4, 4, 2, 2, 2, 2):
        sems += [dma((2, size)), dma((2, size))]
    sems += [dma((8,)), dma((8,)), dma((4,)), dma((4,)), dma((4,)), dma((4,))]
    sems += [dma((2, 8)), dma((2, 4)), dma((2, 4)), dma((2,))]
    shape = (2, 2, 2, 8, 2, 2, BROWS, BLK)
    hbm = pl.BlockSpec(memory_space=pl.ANY)
    return pl.pallas_call(
        exchange_kernel,
        out_shape=(
            jax.ShapeDtypeStruct((ROWS, BLK, JW, C), BF16),
            jax.ShapeDtypeStruct(shape, BF16),
        ),
        in_specs=[hbm, hbm] + [pl.BlockSpec(memory_space=pltpu.VMEM)] * 3,
        out_specs=(hbm, hbm),
        scratch_shapes=[
            pltpu.VMEM(shape, BF16),
            pltpu.VMEM((BLK, COLS, C), BF16),
            pltpu.VMEM((4096, C), F32),
            pltpu.VMEM((H * 32, BLK), F32),
            pltpu.VMEM((BROWS, BLK), BF16),
        ]
        + sems,
        compiler_params=pltpu.CompilerParams(
            collective_id=0, has_side_effects=True, vmem_limit_bytes=60 * 1024 * 1024
        ),
        name="exchange",
    )(x.reshape(BLK, ROWS, JW, C), x, gain, shift, wb)


def return_kernel(y_ref, o_ref, send, recv, local_sem):
    row = lax.axis_index("row")
    xl, y = row // 4, lax.rem(row, 4)
    barrier = pltpu.get_barrier_semaphore()
    for d in range(1, ROWS):
        pl.semaphore_signal(
            barrier, inc=1, device_id={"row": lax.rem(row + d, ROWS)}, device_id_type=MESH
        )
    keep = pltpu.make_async_copy(y_ref.at[row], o_ref.at[:, row], local_sem)
    keep.start()
    pl.semaphore_wait(barrier, ROWS - 1)

    def at(dx, dy):
        return lax.rem(xl + dx, 2) * 4 + lax.rem(y + dy + 4, 4)

    def copy(dx, dy, arriving=False):
        peer = at(dx, -dy if arriving else dy)
        return pltpu.make_async_remote_copy(
            src_ref=y_ref.at[peer],
            dst_ref=o_ref.at[:, peer if arriving else row],
            send_sem=send.at[dx * 4 + dy],
            recv_sem=recv.at[dx * 4 + dy],
            device_id={"row": peer},
            device_id_type=MESH,
        )

    ways = ((1, 2), (1, 1), (1, 3), (0, 2), (1, 0), (0, 1), (0, 3))
    for dx, dy in ways:
        copy(dx, dy).start()
    for dx, dy in ways:
        copy(dx, dy).wait_send()
        copy(dx, dy, True).wait_recv()
    keep.wait()


def send_back(y):
    dma = pltpu.SemaphoreType.DMA
    return pl.pallas_call(
        return_kernel,
        out_shape=jax.ShapeDtypeStruct((BLK, ROWS, JW, C), BF16),
        in_specs=[pl.BlockSpec(memory_space=pl.ANY)],
        out_specs=pl.BlockSpec(memory_space=pl.ANY),
        scratch_shapes=[dma((8,)), dma((8,)), dma],
        compiler_params=pltpu.CompilerParams(
            collective_id=1, has_side_effects=True, vmem_limit_bytes=60 * 1024 * 1024
        ),
        name="send_back",
    )(y)


def attend_kernel(
    valid_ref, x_ref, bg_ref, gain_ref, shift_ref, wp_ref, gb_ref, wo_ref, ob_ref, out_ref,
    bgv, q_s, e_s, k_s, kp_s, v_s, one_s, g_s, tq, tk, tv, tg, p0, p1, p2, p3, acc0, acc1, acc2, acc3, u_s, mx_s, top_s,
    idx_s, bias_sem,
):
    ps, accs = (p0, p1, p2, p3), (acc0, acc1, acc2, acc3)
    col = lax.axis_index("col")
    present = valid_ref[col // 4]

    def place(b, count):
        idx_s[count] = b
        return count + valid_ref[b]

    n = lax.fori_loop(0, 8, place, 0)
    idx_s[n] = 0
    pairs = (n + 1) // 2
    lanes = lax.broadcasted_iota(jnp.int32, (BLK, C), 1)

    def bias_copy(step):
        sk, si = step // n, lax.rem(step, n)
        rk, ri = idx_s[sk], idx_s[si]
        return pltpu.make_async_copy(
            bg_ref.at[rk // 4, lax.rem(rk, 4) // 2, lax.rem(rk, 2), ri], bgv.at[sk, si], bias_sem.at[sk * 8 + si]
        )

    @pl.when(present == 0)
    def _():
        out_ref[...] = x_ref[...]

    @pl.when(present != 0)
    def _():
        def fetch(step, carry):
            bias_copy(step).start()
            return carry

        lax.fori_loop(0, n * n, fetch, 0)
        top_s[...] = jnp.zeros_like(top_s)
        for h in range(H):
            one_s[h * 256 : (h + 1) * 256, :] = jnp.where(
                lax.broadcasted_iota(jnp.int32, (256, C), 1) // HD == h, 1.0, 0.0
            ).astype(BF16)

        def prepare(s, carry):
            r = idx_s[s]
            tok = pl.multiple_of(r * 512, 512)
            x = x_ref[pl.ds(tok, 512), :].astype(F32)
            normed = layer_norm(x, gain_ref[...], shift_ref[...])
            proj = dot_nn(normed, wp_ref[...])
            q = (proj[:, :C] * (HD ** -0.5)).astype(BF16)
            k = proj[:, C : 2 * C].astype(BF16)
            tq[...] = q.astype(F32)
            tk[...] = k.astype(F32)
            tv[...] = proj[:, 2 * C : 3 * C]
            tg[...] = jax.nn.sigmoid(proj[:, 3 * C :] + gb_ref[...])
            heads = (
                lax.broadcasted_iota(jnp.int32, (C, C), 0) // HD
                == lax.broadcasted_iota(jnp.int32, (C, C), 1) // HD
            ).astype(BF16)
            q2 = dot_nn(q * q, heads)
            k2 = dot_nn(k * k, heads)
            top_s[0] = jnp.maximum(top_s[0], jnp.max(q2.reshape(64, 8, C), axis=0))
            top_s[1] = jnp.maximum(top_s[1], jnp.max(k2.reshape(64, 8, C), axis=0))
            at = pl.multiple_of(s * BLK, BLK)
            it = s // 2
            sub = pl.multiple_of(lax.rem(s, 2) * BLK, BLK)
            for j in range(JW):
                qj = tq[pl.ds(j, BLK, stride=JW), :].astype(BF16)
                vj = tv[pl.ds(j, BLK, stride=JW), :].astype(BF16)
                k_s[j, pl.ds(at, BLK), :] = tk[pl.ds(j, BLK, stride=JW), :].astype(BF16)
                g_s[j, pl.ds(at, BLK), :] = tg[pl.ds(j, BLK, stride=JW), :]
                for h in range(H):
                    pick = one_s[h * 256 : h * 256 + BLK, :]
                    q_s[j, it, h, pl.ds(sub, BLK), :] = qj * pick
                    v_s[j, it, pl.ds(h * 256 + sub, BLK), :] = vj * pick
            kp_s[pl.ds(at, BLK), :] = jnp.where(
                (lanes // 8 == s) | (lanes // 8 == 8), 1.0, 0.0
            ).astype(BF16)
            return carry

        lax.fori_loop(0, n, prepare, 0)

        def fetched(step, carry):
            bias_copy(step).wait()
            return carry

        lax.fori_loop(0, n * n, fetched, 0)

        def centre(s, carry):
            tiles = []
            high = jnp.full((8, BLK), NEG, F32)
            for b in range(8):
                part = bgv[b, s, 0, 0, H * 32 :, :].astype(F32)
                for q4 in range(1, 4):
                    part = part + bgv[b, s, q4 // 2, q4 % 2, H * 32 :, :].astype(F32)
                tiles.append(jnp.where(b < n, part, 0.0))
                high = jnp.maximum(high, jnp.where(b < n, part, NEG))
            tiles.append(-high)
            tiles.append(jnp.full((8, BLK), NEG, F32))
            tiles.append(jnp.zeros((48, BLK), F32))
            turned = jnp.concatenate(tiles, axis=0).T
            it = s // 2
            sub = pl.multiple_of(lax.rem(s, 2) * BLK, BLK)
            for h in range(H):
                e_s[it, h, pl.ds(sub, BLK), :] = jnp.where(
                    ((lax.rem(lanes, 8) == h) & (lanes < 72)) | (lanes == 72), turned, 0.0
                ).astype(BF16)
            return carry

        lax.fori_loop(0, n, centre, 0)

        @pl.when(lax.rem(n, 2) == 1)
        def _():
            at = pl.multiple_of(n * BLK, BLK)
            it = n // 2
            zero = jnp.zeros((BLK, C), BF16)
            kp_s[pl.ds(at, BLK), :] = jnp.where(lanes == 72, 1.0, 0.0).astype(BF16)
            for j in range(JW):
                k_s[j, pl.ds(at, BLK), :] = zero
                for h in range(H):
                    v_s[j, it, h * 256 + BLK : h * 256 + 256, :] = zero
                    q_s[j, it, h, BLK : 2 * BLK, :] = zero
            for h in range(H):
                e_s[it, h, BLK : 2 * BLK, :] = zero

        bound = jnp.max(jnp.max(top_s[0], axis=0, keepdims=True) * jnp.max(top_s[1], axis=0, keepdims=True))

        def scores(j, it, kt, h):
            keys = pl.ds(pl.multiple_of(kt * 256, 256), 256)
            s = dot_nt(
                jnp.concatenate([q_s[j, it, h], e_s[it, h]], axis=1),
                jnp.concatenate([k_s[j, keys, :], kp_s[keys, :]], axis=1),
            )
            rows = []
            for a in range(2):
                si = jnp.minimum(it * 2 + a, n - 1)
                parts = []
                for b in range(2):
                    sk = jnp.minimum(kt * 2 + b, n - 1)
                    bias = bgv[sk, si, :, :, h * 32 : h * 32 + 32, :]
                    parts.append(
                        s[a * BLK : (a + 1) * BLK, b * BLK : (b + 1) * BLK]
                        + bias.reshape(BLK, BLK).astype(F32)
                    )
                rows.append(jnp.concatenate(parts, axis=1))
            return jnp.concatenate(rows, axis=0)

        def weigh(p_ref, j, it, kt, shifted):
            for h in range(H):
                s = scores(j, it, kt, h)
                if shifted:
                    s = s - mx_s[h][:, 0:1]
                p_ref[:, h * 256 : (h + 1) * 256] = jnp.exp(s).astype(BF16)

        def gather_values(p_ref, j, kt, to_ref, from_ref):
            got = dot_nn(p_ref[...], jnp.concatenate([v_s[j, kt], one_s[...]], axis=1))
            to_ref[...] = jnp.where(kt == 0, 0.0, from_ref[...]) + got

        def finish(j, it, acc):
            base = pl.multiple_of(it * 256, 256)
            mixed = (acc[:, 0:C] / acc[:, C : 2 * C]).astype(BF16).astype(F32)
            gated = (g_s[j, pl.ds(base, 256), :] * mixed).astype(BF16)
            update = dot_nn(gated, wo_ref[...]) + ob_ref[...]
            for a in range(2):
                ri = idx_s[it * 2 + a]

                @pl.when(it * 2 + a < n)
                def _():
                    u_s[pl.ds(ri * 512 + j, BLK, stride=JW), :] = update[a * BLK : (a + 1) * BLK]

        def four_columns(step, carry):
            it, kt = step // pairs, lax.rem(step, pairs)
            before = jnp.maximum(step - 1, 0)
            it0, kt0 = before // pairs, lax.rem(before, pairs)
            weigh(ps[0], 0, it, kt, False)
            gather_values(ps[3], 3, kt0, accs[3], accs[3])
            for j in range(1, JW):
                weigh(ps[j], j, it, kt, False)
                gather_values(ps[j - 1], j - 1, kt, accs[j - 1], accs[j - 1])

            @pl.when((kt0 == pairs - 1) & (step > 0))
            def _():
                finish(3, it0, accs[3])

            @pl.when(kt == pairs - 1)
            def _():
                for j in range(3):
                    finish(j, it, accs[j])

            return carry

        def over_tiles_shifted(step, carry):
            j, it = step // pairs, lax.rem(step, pairs)
            mx_s[...] = jnp.full_like(mx_s, NEG)

            def highest(kt, inner):
                for h in range(H):
                    top = jnp.max(scores(j, it, kt, h), axis=-1, keepdims=True)
                    mx_s[h] = jnp.maximum(mx_s[h], top)
                return inner

            def sum_up(kt, inner):
                weigh(p0, j, it, kt, True)
                gather_values(p0, j, kt, acc0, acc0)
                return inner

            lax.fori_loop(0, pairs, highest, 0)
            lax.fori_loop(0, pairs, sum_up, 0)
            finish(j, it, acc0)
            return carry

        @pl.when(bound <= 3000.0)
        def _():
            lax.fori_loop(0, pairs * pairs, four_columns, 0)
            gather_values(ps[3], 3, pairs - 1, accs[3], accs[3])
            finish(3, pairs - 1, accs[3])

        @pl.when(jnp.logical_not(bound <= 3000.0))
        def _():
            lax.fori_loop(0, pairs * JW, over_tiles_shifted, 0)

        def write(r, carry):
            tok = pl.ds(pl.multiple_of(r * 512, 512), 512)

            @pl.when(valid_ref[r] > 0)
            def _():
                out_ref[tok, :] = (x_ref[tok, :].astype(F32) + u_s[tok, :]).astype(BF16)

            @pl.when(valid_ref[r] == 0)
            def _():
                out_ref[tok, :] = x_ref[tok, :]

            return carry

        lax.fori_loop(0, 8, write, 0)


def attend(x, bg, gain, shift, wp, gb, wo, ob, valid):
    vmem = pl.BlockSpec(memory_space=pltpu.VMEM)
    v = pltpu.VMEM
    return pl.pallas_call(
        attend_kernel,
        out_shape=jax.ShapeDtypeStruct((4096, C), BF16),
        in_specs=[pl.BlockSpec(memory_space=pltpu.SMEM), vmem, pl.BlockSpec(memory_space=pl.ANY)]
        + [vmem] * 6,
        out_specs=vmem,
        scratch_shapes=[
            v((8, 8, 2, 2, BROWS, BLK), BF16),
            v((JW, 4, H, 256, C), BF16),
            v((4, H, 256, C), BF16),
            v((JW, 1024, C), BF16),
            v((1024, C), BF16),
            v((JW, 4, H * 256, C), BF16),
            v((H * 256, C), BF16),
            v((JW, 1024, C), F32),
            v((512, C), F32), v((512, C), F32), v((512, C), F32), v((512, C), F32),
            v((256, H * 256), BF16), v((256, H * 256), BF16), v((256, H * 256), BF16), v((256, H * 256), BF16),
            v((256, 256), F32), v((256, 256), F32), v((256, 256), F32), v((256, 256), F32),
            v((4096, C), F32),
            v((H, 256, C), F32),
            v((2, 8, C), F32),
            pltpu.SMEM((16,), jnp.int32),
            pltpu.SemaphoreType.DMA((64,)),
        ],
        compiler_params=pltpu.CompilerParams(vmem_limit_bytes=60 * 1024 * 1024),
        name="attend",
    )(valid, x, bg, gain, shift, wp, gb, wo, ob)


def shards(pair_rep, ln_gain, ln_shift, w_proj, gate_bias, w_bias, w_out, out_bias, block_valid):
    gain, shift = ln_gain[None], ln_shift[None]
    columns, bias = exchange(pair_rep, gain, shift, w_bias.T)
    y = attend(
        columns.reshape(4096, C), bias, gain, shift, w_proj, gate_bias[None], w_out, out_bias[None],
        block_valid,
    )
    out = send_back(y.reshape(ROWS, BLK, JW, C))
    return out.reshape(BLK, COLS, C)


def solution(mesh):
    return jax.shard_map(
        shards,
        mesh=mesh,
        in_specs=(P("row", "col", None), P(), P(), P(), P(), P(), P(), P(), P()),
        out_specs=P("row", "col", None),
        check_vma=False,
    )
```

```python
import jax
import jax.numpy as jnp
from jax import lax
from jax.experimental import pallas as pl
from jax.experimental.pallas import tpu as pltpu
from jax.sharding import PartitionSpec as P

H = 4
HD = 32
C = 128
ROWS = 8
COLS = 32
BLK = 128
JW = 4
BROWS = H * 32 + 8
COLOR_Z = (0, 64)
COLOR_Y = (64, 96)
COLOR_X = (96, 136)
MESH = pl.DeviceIdType.MESH
F32 = jnp.float32
BF16 = jnp.bfloat16
NEG = -1e30


def dot_nt(a, b):
    return lax.dot_general(a, b, (((1,), (1,)), ((), ())), preferred_element_type=F32)


def dot_nn(a, b):
    return lax.dot_general(a, b, (((1,), (0,)), ((), ())), preferred_element_type=F32)


def layer_norm(x, gain, shift):
    average = jnp.mean(x, axis=-1, keepdims=True)
    centred = x - average
    spread = jnp.mean(centred * centred, axis=-1, keepdims=True)
    return (centred * lax.rsqrt(spread + 1e-05) * gain + shift).astype(BF16)


def normalise_block(xv, gain_ref, shift_ref, n_s):
    def norm(step, carry):
        x = xv[pl.ds(step * 16, 16), :, :].astype(F32).reshape(512, C)
        n_s[pl.ds(pl.multiple_of(step * 512, 512), 512), :] = layer_norm(
            x, gain_ref[...], shift_ref[...]
        ).astype(F32)
        return carry

    lax.fori_loop(0, 8, norm, 0)


def bias_block(wb_ref, n_s, b_s, blk_ref, col):
    wide = wb_ref[...].astype(F32)
    wide = jnp.concatenate([wide, jnp.zeros((8 - H, C), F32)], axis=0).astype(BF16)
    lanes = lax.broadcasted_iota(jnp.int32, (8, BLK), 1)
    first = lax.rem(col, 4) * 32
    centres = jnp.zeros((8, BLK), F32)
    for i in range(32):
        part = dot_nt(wide, n_s[pl.ds(i, BLK, stride=32), :].astype(BF16))
        centre = jnp.max(part, axis=-1, keepdims=True).astype(BF16).astype(F32)
        part = part - centre
        for h in range(H):
            b_s[h * 32 + i : h * 32 + i + 1, :] = part[h : h + 1, :]
        centres = jnp.where(lanes == first + i, centre, centres)
    blk_ref[0 : H * 32, :] = b_s[...].astype(BF16)
    blk_ref[H * 32 :, :] = centres.astype(BF16)


class Ring:
    def __init__(self, size, mine, unit, at, send, recv):
        self.size, self.mine, self.unit, self.at, self.send, self.recv = size, mine, unit, at, send, recv
        self.last = size // 2

    def copy(self, way, step, place):
        half = way if step == self.last else None
        sign = 1 - 2 * way
        return pltpu.make_async_remote_copy(
            src_ref=self.unit(place, half),
            dst_ref=self.unit(place, half),
            send_sem=self.send.at[way, step - 1],
            recv_sem=self.recv.at[way, step - 1],
            device_id=self.at(lax.rem(self.mine + sign + self.size, self.size)),
            device_id_type=MESH,
        )

    def away(self, way, steps):
        return lax.rem(self.mine - (1 - 2 * way) * steps + self.size, self.size)

    def hop(self, way, step):
        return self.copy(way, step, self.away(way, step - 1))

    def arrival(self, way, step):
        return self.copy(way, step, self.away(way, step))


def exchange_kernel(
    x_ref, flat_ref, gain_ref, shift_ref, wb_ref, o_ref, bg_out,
    bg, xv, n_s, b_s, blk_ref, a_send, a_recv, pz_send, pz_recv, pq_send, pq_recv,
    r0s, r0r, r1s, r1r, r2s, r2r, r3s, r3r, r4s, r4r, r5s, r5r, r6s, r6r, r7s, r7r,
    r8s, r8r, r9s, r9r, ras, rar, rbs, rbr,
    dz_send, dz_recv, dy_send, dy_recv, dx_send, dx_recv, cz, cy, cx, own_sem,
):
    row = lax.axis_index("row")
    col = lax.axis_index("col")
    xl, y = row // 4, lax.rem(row, 4)
    z, xh, core = col // 4, lax.rem(col // 2, 2), lax.rem(col, 2)
    x = xh * 2 + xl
    every = slice(None)
    block_in = pltpu.make_async_copy(flat_ref, xv, own_sem.at[1])
    block_in.start()

    def device(x_, y_, z_, core_=None):
        core_ = core if core_ is None else core_
        return {"row": lax.rem(x_, 2) * 4 + y_, "col": z_ * 4 + (x_ // 2) * 2 + core_}

    rows_z = pl.ds(COLOR_Z[0], COLOR_Z[1] - COLOR_Z[0])
    rows_y = pl.ds(COLOR_Y[0], COLOR_Y[1] - COLOR_Y[0])
    rows_x = pl.ds(COLOR_X[0], COLOR_X[1] - COLOR_X[0])
    rows_q = pl.ds(COLOR_Y[0], COLOR_X[1] - COLOR_Y[0])

    def part(half, count):
        return every if half is None else pl.ds(half * count, count)

    yh, yl = y // 2, lax.rem(y, 2)

    def unit_zx(p, half):
        return bg.at[lax.rem(p, 2), part(half, 1), :, z, p // 2, rows_z, :]

    def unit_yx(p, half):
        return bg.at[lax.rem(p, 2), yh, yl, part(half, 4), p // 2, rows_y, :]

    def unit_xy(p, half):
        return bg.at[xl, p // 2, lax.rem(p, 2), part(half, 4), xh, rows_x, :]

    def unit_za(p, half):
        return bg.at[xl, part(half, 1), :, p, xh, rows_z, :]

    def unit_zb(p, half):
        return bg.at[1 - xl, part(half, 1), :, p, :, rows_z, :]

    def unit_zc(p, half):
        return bg.at[xl, part(half, 1), :, p, 1 - xh, rows_z, :]

    def unit_ya(p, half):
        return bg.at[xl, p // 2, lax.rem(p, 2), part(half, 4), xh, rows_y, :]

    def unit_yb(p, half):
        return bg.at[1 - xl, p // 2, lax.rem(p, 2), part(half, 4), :, rows_y, :]

    def unit_yc(p, half):
        return bg.at[xl, p // 2, lax.rem(p, 2), part(half, 4), 1 - xh, rows_y, :]

    def unit_xa(p, half):
        return bg.at[lax.rem(p, 2), yh, yl, part(half, 4), p // 2, rows_x, :]

    def unit_xb(p, half):
        return bg.at[lax.rem(p, 2), :, 1 - yl, part(half, 4), p // 2, rows_x, :]

    def unit_xc(p, half):
        return bg.at[lax.rem(p, 2), 1 - yh, yl, part(half, 4), p // 2, rows_x, :]

    def unit_z(p, half, ref=None, side=None):
        if ref is None:
            return bg.at[:, :, :, p, :, rows_z, :]
        return ref.at[:, :, :, p, :, side, rows_z, :]

    def unit_y(p, half, ref=None, side=None):
        if ref is None:
            return bg.at[:, p // 2, lax.rem(p, 2), :, :, rows_y, :]
        return ref.at[:, p // 2, lax.rem(p, 2), :, :, side, rows_y, :]

    def unit_x(p, half, ref=None, side=None):
        if ref is None:
            return bg.at[lax.rem(p, 2), :, :, :, p // 2, rows_x, :]
        return ref.at[lax.rem(p, 2), :, :, :, p // 2, side, rows_x, :]

    along_x = lambda p: device(p, y, z)
    along_y = lambda p: device(x, p, z)
    along_z = lambda p: device(x, y, p)
    zx = Ring(4, x, unit_zx, along_x, r0s, r0r)
    yx = Ring(4, x, unit_yx, along_x, r1s, r1r)
    xy = Ring(4, y, unit_xy, along_y, r2s, r2r)
    za = Ring(8, z, unit_za, along_z, r3s, r3r)
    zb = Ring(8, z, unit_zb, along_z, r6s, r6r)
    zc = Ring(8, z, unit_zc, along_z, r7s, r7r)
    ya = Ring(4, y, unit_ya, along_y, r4s, r4r)
    yb = Ring(4, y, unit_yb, along_y, r8s, r8r)
    yc = Ring(4, y, unit_yc, along_y, r9s, r9r)
    xa = Ring(4, x, unit_xa, along_x, r5s, r5r)
    xb = Ring(4, x, unit_xb, along_x, ras, rar)
    xc = Ring(4, x, unit_xc, along_x, rbs, rbr)
    rz = Ring(8, z, unit_z, along_z, None, None)
    ry = Ring(4, y, unit_y, along_y, None, None)
    rx = Ring(4, x, unit_x, along_x, None, None)
    finals = ((rz, dz_send, dz_recv, cz), (ry, dy_send, dy_recv, cy), (rx, dx_send, dx_recv, cx))

    def round_line(mine, size, act):
        def body(d, carry):
            act(lax.rem(mine + d, size))
            return carry

        lax.fori_loop(1, size, body, 0)

    barrier = pltpu.get_barrier_semaphore()

    def greet(target):
        pl.semaphore_signal(barrier, inc=1, device_id=target, device_id_type=MESH)

    round_line(z, 8, lambda p: greet(device(x, y, p)))
    round_line(x, 4, lambda p: greet(device(p, y, z)))
    round_line(row, ROWS, lambda p: greet({"row": p, "col": col}))
    greet(device(x, y, z, 1 - core))
    block_in.wait()
    normalise_block(xv, gain_ref, shift_ref, n_s)
    pl.semaphore_wait(barrier, 18)

    def line_z(p, sender):
        return pltpu.make_async_remote_copy(
            src_ref=blk_ref.at[rows_z, :],
            dst_ref=bg.at[xl, sender // 2, lax.rem(sender, 2), z, xh, rows_z, :],
            send_sem=pz_send.at[p],
            recv_sem=pz_recv.at[sender],
            device_id=device(x, p, z),
            device_id_type=MESH,
        )

    def line_q(p, sender):
        return pltpu.make_async_remote_copy(
            src_ref=blk_ref.at[rows_q, :],
            dst_ref=bg.at[xl, yh, yl, sender, xh, rows_q, :],
            send_sem=pq_send.at[p],
            recv_sem=pq_recv.at[sender],
            device_id=device(x, y, p),
            device_id_type=MESH,
        )


    def column(dx, dy, arriving=False):
        sign = -1 if arriving else 1
        px, py = lax.rem(xl + dx, 2), lax.rem(y + sign * dy + 4, 4)
        peer = px * 4 + py
        return pltpu.make_async_remote_copy(
            src_ref=x_ref.at[:, peer],
            dst_ref=o_ref.at[peer if arriving else row],
            send_sem=a_send.at[dx * 4 + dy],
            recv_sem=a_recv.at[dx * 4 + dy],
            device_id={"row": peer, "col": col},
            device_id_type=MESH,
        )

    keep = pltpu.make_async_copy(x_ref.at[:, row], o_ref.at[row], own_sem.at[0])
    keep.start()
    early = ()
    late = ((1, 0), (0, 1), (0, 3), (1, 1), (1, 3), (0, 2), (1, 2))
    for dx, dy in early:
        column(dx, dy).start()
    bias_block(wb_ref, n_s, b_s, blk_ref, col)
    bg[xl, yh, yl, z, xh] = blk_ref[...]
    round_line(y, 4, lambda p: line_z(p, y).start())
    round_line(z, 8, lambda p: line_q(p, z).start())

    def launch(ring, step):
        for way in (0, 1):
            ring.hop(way, step).start()

    def await_step(ring, step):
        for way in (0, 1):
            ring.arrival(way, step).wait_recv()

    def across(final, place):
        ring, send, recv, _ = final
        return pltpu.make_async_remote_copy(
            src_ref=ring.unit(place, None),
            dst_ref=ring.unit(place, None, bg_out, core),
            send_sem=send.at[place],
            recv_sem=recv.at[place],
            device_id=device(x, y, z, 1 - core),
            device_id_type=MESH,
        )

    def across_arrival(final, place):
        ring, send, recv, _ = final
        return pltpu.make_async_remote_copy(
            src_ref=ring.unit(place, None),
            dst_ref=ring.unit(place, None, bg_out, 1 - core), send_sem=send.at[place], recv_sem=recv.at[place],
            device_id=device(x, y, z, 1 - core), device_id_type=MESH,
        )

    def keep_unit(final, place):
        ring, _, _, sem = final
        return pltpu.make_async_copy(
            ring.unit(place, None), ring.unit(place, None, bg_out, core), sem.at[place]
        )

    def hand_on(final, place):
        across(final, place).start()
        keep_unit(final, place).start()

    def onward(ring, step):
        for way in (0, 1):
            ring.arrival(way, step).wait_recv()
            if step < ring.last:
                ring.hop(way, step + 1).start()

    def hand_unit(which, step):
        ring = finals[which][0]
        hand_on(finals[which], ring.away(0, step))
        if step < ring.last:
            hand_on(finals[which], ring.away(1, step))

    round_line(y, 4, lambda p: line_z(p, p).wait_recv())
    launch(zx, 1)
    launch(za, 1)
    await_step(zx, 1)
    launch(zx, 2)
    launch(zb, 1)
    round_line(z, 8, lambda p: line_q(p, p).wait_recv())
    launch(yx, 1)
    launch(xy, 1)
    launch(xa, 1)
    launch(ya, 1)
    onward(za, 1)
    await_step(zx, 2)
    launch(zc, 1)
    hand_on(finals[0], z)
    await_step(xy, 1)
    launch(xy, 2)
    launch(xb, 1)
    await_step(yx, 1)
    launch(yx, 2)
    launch(yb, 1)
    onward(zb, 1)
    await_step(xy, 2)
    launch(xc, 1)
    hand_on(finals[2], x)
    await_step(yx, 2)
    launch(yc, 1)
    hand_on(finals[1], y)
    onward(xa, 1)
    onward(ya, 1)
    onward(za, 2)
    onward(zc, 1)
    hand_unit(0, 1)
    onward(xb, 1)
    onward(yb, 1)
    onward(zb, 2)
    onward(xc, 1)
    hand_unit(2, 1)
    onward(yc, 1)
    hand_unit(1, 1)
    column(1, 0).start()
    column(0, 1).start()
    column(0, 3).start()
    column(1, 1).start()
    column(1, 3).start()
    column(0, 2).start()
    column(1, 2).start()
    onward(za, 3)
    onward(zc, 2)
    hand_unit(0, 2)
    onward(xa, 2)
    onward(xb, 2)
    onward(xc, 2)
    hand_unit(2, 2)
    onward(ya, 2)
    onward(yb, 2)
    onward(yc, 2)
    hand_unit(1, 2)
    onward(zb, 3)
    onward(za, 4)
    onward(zc, 3)
    hand_unit(0, 3)
    onward(zb, 4)
    onward(zc, 4)
    hand_unit(0, 4)

    for final in (finals[1], finals[2], finals[0]):
        ring = final[0]
        for d in range(ring.size):
            place = ring.away(d % 2, (d + 1) // 2)
            across_arrival(final, place).wait_recv()
    round_line(y, 4, lambda p: line_z(p, y).wait_send())
    round_line(z, 8, lambda p: line_q(p, z).wait_send())
    for ring in (zx, yx, xy, za, zb, zc, ya, yb, yc, xa, xb, xc):
        for way in (0, 1):
            for step in range(1, ring.last + 1):
                ring.hop(way, step).wait_send()
    for dx, dy in early + late:
        column(dx, dy).wait_send()
        column(dx, dy, True).wait_recv()
    keep.wait()
    for final in finals:
        for place in range(final[0].size):
            across(final, place).wait_send()
            keep_unit(final, place).wait()


def exchange(x, gain, shift, wb):
    dma = pltpu.SemaphoreType.DMA
    sems = [dma((8,)), dma((8,)), dma((4,)), dma((4,)), dma((8,)), dma((8,))]
    for size in (2, 2, 2, 4, 2, 2, 4, 4, 2, 2, 2, 2):
        sems += [dma((2, size)), dma((2, size))]
    sems += [dma((8,)), dma((8,)), dma((4,)), dma((4,)), dma((4,)), dma((4,))]
    sems += [dma((8,)), dma((4,)), dma((4,)), dma((2,))]
    shape = (2, 2, 2, 8, 2, 2, BROWS, BLK)
    hbm = pl.BlockSpec(memory_space=pl.ANY)
    return pl.pallas_call(
        exchange_kernel,
        out_shape=(
            jax.ShapeDtypeStruct((ROWS, BLK, JW, C), BF16),
            jax.ShapeDtypeStruct(shape, BF16),
        ),
        in_specs=[hbm, hbm] + [pl.BlockSpec(memory_space=pltpu.VMEM)] * 3,
        out_specs=(hbm, hbm),
        scratch_shapes=[
            pltpu.VMEM(shape[:5] + shape[6:], BF16),
            pltpu.VMEM((BLK, COLS, C), BF16),
            pltpu.VMEM((4096, C), F32),
            pltpu.VMEM((H * 32, BLK), F32),
            pltpu.VMEM((BROWS, BLK), BF16),
        ]
        + sems,
        compiler_params=pltpu.CompilerParams(
            collective_id=0, has_side_effects=True, vmem_limit_bytes=60 * 1024 * 1024
        ),
        name="exchange",
    )(x.reshape(BLK, ROWS, JW, C), x, gain, shift, wb)


def return_kernel(y_ref, o_ref, send, recv, local_sem):
    row = lax.axis_index("row")
    xl, y = row // 4, lax.rem(row, 4)
    barrier = pltpu.get_barrier_semaphore()
    for d in range(1, ROWS):
        pl.semaphore_signal(
            barrier, inc=1, device_id={"row": lax.rem(row + d, ROWS)}, device_id_type=MESH
        )
    keep = pltpu.make_async_copy(y_ref.at[row], o_ref.at[:, row], local_sem)
    keep.start()
    pl.semaphore_wait(barrier, ROWS - 1)

    def at(dx, dy):
        return lax.rem(xl + dx, 2) * 4 + lax.rem(y + dy + 4, 4)

    def copy(dx, dy, arriving=False):
        peer = at(dx, -dy if arriving else dy)
        return pltpu.make_async_remote_copy(
            src_ref=y_ref.at[peer],
            dst_ref=o_ref.at[:, peer if arriving else row],
            send_sem=send.at[dx * 4 + dy],
            recv_sem=recv.at[dx * 4 + dy],
            device_id={"row": peer},
            device_id_type=MESH,
        )

    ways = ((1, 2), (1, 1), (1, 3), (0, 2), (1, 0), (0, 1), (0, 3))
    for dx, dy in ways:
        copy(dx, dy).start()
    for dx, dy in ways:
        copy(dx, dy).wait_send()
        copy(dx, dy, True).wait_recv()
    keep.wait()


def send_back(y):
    dma = pltpu.SemaphoreType.DMA
    return pl.pallas_call(
        return_kernel,
        out_shape=jax.ShapeDtypeStruct((BLK, ROWS, JW, C), BF16),
        in_specs=[pl.BlockSpec(memory_space=pl.ANY)],
        out_specs=pl.BlockSpec(memory_space=pl.ANY),
        scratch_shapes=[dma((8,)), dma((8,)), dma],
        compiler_params=pltpu.CompilerParams(
            collective_id=1, has_side_effects=True, vmem_limit_bytes=60 * 1024 * 1024
        ),
        name="send_back",
    )(y)


def attend_kernel(
    valid_ref, x_ref, bg_ref, gain_ref, shift_ref, wp_ref, gb_ref, wo_ref, ob_ref, out_ref,
    bgv, q_s, e_s, k_s, kp_s, v_s, one_s, g_s, tq, tk, tv, tg, p0, p1, p2, p3, acc0, acc1, acc2, acc3, u_s, mx_s, top_s,
    idx_s, bias_sem,
):
    ps, accs = (p0, p1, p2, p3), (acc0, acc1, acc2, acc3)
    col = lax.axis_index("col")
    present = valid_ref[col // 4]

    def place(b, count):
        idx_s[count] = b
        return count + valid_ref[b]

    n = lax.fori_loop(0, 8, place, 0)
    idx_s[n] = 0
    pairs = (n + 1) // 2
    lanes = lax.broadcasted_iota(jnp.int32, (BLK, C), 1)

    def bias_copy(step):
        sk, si = step // n, lax.rem(step, n)
        rk, ri = idx_s[sk], idx_s[si]
        return pltpu.make_async_copy(
            bg_ref.at[rk // 4, lax.rem(rk, 4) // 2, lax.rem(rk, 2), ri], bgv.at[sk, si], bias_sem.at[sk * 8 + si]
        )

    @pl.when(present == 0)
    def _():
        out_ref[...] = x_ref[...]

    @pl.when(present != 0)
    def _():
        def fetch(step, carry):
            bias_copy(step).start()
            return carry

        lax.fori_loop(0, n * n, fetch, 0)
        top_s[...] = jnp.zeros_like(top_s)
        for h in range(H):
            one_s[h * 256 : (h + 1) * 256, :] = jnp.where(
                lax.broadcasted_iota(jnp.int32, (256, C), 1) // HD == h, 1.0, 0.0
            ).astype(BF16)

        def prepare(s, carry):
            r = idx_s[s]
            tok = pl.multiple_of(r * 512, 512)
            x = x_ref[pl.ds(tok, 512), :].astype(F32)
            normed = layer_norm(x, gain_ref[...], shift_ref[...])
            proj = dot_nn(normed, wp_ref[...])
            q = (proj[:, :C] * (HD ** -0.5)).astype(BF16)
            k = proj[:, C : 2 * C].astype(BF16)
            tq[...] = q.astype(F32)
            tk[...] = k.astype(F32)
            tv[...] = proj[:, 2 * C : 3 * C]
            tg[...] = jax.nn.sigmoid(proj[:, 3 * C :] + gb_ref[...])
            heads = (
                lax.broadcasted_iota(jnp.int32, (C, C), 0) // HD
                == lax.broadcasted_iota(jnp.int32, (C, C), 1) // HD
            ).astype(BF16)
            q2 = dot_nn(q * q, heads)
            k2 = dot_nn(k * k, heads)
            top_s[0] = jnp.maximum(top_s[0], jnp.max(q2.reshape(64, 8, C), axis=0))
            top_s[1] = jnp.maximum(top_s[1], jnp.max(k2.reshape(64, 8, C), axis=0))
            at = pl.multiple_of(s * BLK, BLK)
            it = s // 2
            sub = pl.multiple_of(lax.rem(s, 2) * BLK, BLK)
            for j in range(JW):
                qj = tq[pl.ds(j, BLK, stride=JW), :].astype(BF16)
                vj = tv[pl.ds(j, BLK, stride=JW), :].astype(BF16)
                k_s[j, pl.ds(at, BLK), :] = tk[pl.ds(j, BLK, stride=JW), :].astype(BF16)
                g_s[j, pl.ds(at, BLK), :] = tg[pl.ds(j, BLK, stride=JW), :]
                for h in range(H):
                    pick = one_s[h * 256 : h * 256 + BLK, :]
                    q_s[j, it, h, pl.ds(sub, BLK), :] = qj * pick
                    v_s[j, it, pl.ds(h * 256 + sub, BLK), :] = vj * pick
            kp_s[pl.ds(at, BLK), :] = jnp.where(
                (lanes // 8 == s) | (lanes // 8 == 8), 1.0, 0.0
            ).astype(BF16)
            return carry

        lax.fori_loop(0, n, prepare, 0)

        def fetched(step, carry):
            bias_copy(step).wait()
            return carry

        lax.fori_loop(0, n * n, fetched, 0)

        def centre(s, carry):
            tiles = []
            high = jnp.full((8, BLK), NEG, F32)
            for b in range(8):
                part = bgv[b, s, 0, 0, H * 32 :, :].astype(F32)
                for q4 in range(1, 4):
                    part = part + bgv[b, s, q4 // 2, q4 % 2, H * 32 :, :].astype(F32)
                tiles.append(jnp.where(b < n, part, 0.0))
                high = jnp.maximum(high, jnp.where(b < n, part, NEG))
            tiles.append(-high)
            tiles.append(jnp.full((8, BLK), NEG, F32))
            tiles.append(jnp.zeros((48, BLK), F32))
            turned = jnp.concatenate(tiles, axis=0).T
            it = s // 2
            sub = pl.multiple_of(lax.rem(s, 2) * BLK, BLK)
            for h in range(H):
                e_s[it, h, pl.ds(sub, BLK), :] = jnp.where(
                    ((lax.rem(lanes, 8) == h) & (lanes < 72)) | (lanes == 72), turned, 0.0
                ).astype(BF16)
            return carry

        lax.fori_loop(0, n, centre, 0)

        @pl.when(lax.rem(n, 2) == 1)
        def _():
            at = pl.multiple_of(n * BLK, BLK)
            it = n // 2
            zero = jnp.zeros((BLK, C), BF16)
            kp_s[pl.ds(at, BLK), :] = jnp.where(lanes == 72, 1.0, 0.0).astype(BF16)
            for j in range(JW):
                k_s[j, pl.ds(at, BLK), :] = zero
                for h in range(H):
                    v_s[j, it, h * 256 + BLK : h * 256 + 256, :] = zero
                    q_s[j, it, h, BLK : 2 * BLK, :] = zero
            for h in range(H):
                e_s[it, h, BLK : 2 * BLK, :] = zero

        bound = jnp.max(jnp.max(top_s[0], axis=0, keepdims=True) * jnp.max(top_s[1], axis=0, keepdims=True))

        def scores(j, it, kt, h):
            keys = pl.ds(pl.multiple_of(kt * 256, 256), 256)
            s = dot_nt(
                jnp.concatenate([q_s[j, it, h], e_s[it, h]], axis=1),
                jnp.concatenate([k_s[j, keys, :], kp_s[keys, :]], axis=1),
            )
            rows = []
            for a in range(2):
                si = jnp.minimum(it * 2 + a, n - 1)
                parts = []
                for b in range(2):
                    sk = jnp.minimum(kt * 2 + b, n - 1)
                    bias = bgv[sk, si, :, :, h * 32 : h * 32 + 32, :]
                    parts.append(
                        s[a * BLK : (a + 1) * BLK, b * BLK : (b + 1) * BLK]
                        + bias.reshape(BLK, BLK).astype(F32)
                    )
                rows.append(jnp.concatenate(parts, axis=1))
            return jnp.concatenate(rows, axis=0)

        def weigh(p_ref, j, it, kt, shifted):
            for h in range(H):
                s = scores(j, it, kt, h)
                if shifted:
                    s = s - mx_s[h][:, 0:1]
                p_ref[:, h * 256 : (h + 1) * 256] = jnp.exp(s).astype(BF16)

        def gather_values(p_ref, j, kt, to_ref, from_ref):
            got = dot_nn(p_ref[...], jnp.concatenate([v_s[j, kt], one_s[...]], axis=1))
            to_ref[...] = jnp.where(kt == 0, 0.0, from_ref[...]) + got

        def finish(j, it, acc):
            base = pl.multiple_of(it * 256, 256)
            mixed = (acc[:, 0:C] / acc[:, C : 2 * C]).astype(BF16).astype(F32)
            gated = (g_s[j, pl.ds(base, 256), :] * mixed).astype(BF16)
            update = dot_nn(gated, wo_ref[...]) + ob_ref[...]
            for a in range(2):
                ri = idx_s[it * 2 + a]

                @pl.when(it * 2 + a < n)
                def _():
                    u_s[pl.ds(ri * 512 + j, BLK, stride=JW), :] = update[a * BLK : (a + 1) * BLK]

        def four_columns(step, carry):
            it, kt = step // pairs, lax.rem(step, pairs)
            before = jnp.maximum(step - 1, 0)
            it0, kt0 = before // pairs, lax.rem(before, pairs)
            weigh(ps[0], 0, it, kt, False)
            gather_values(ps[3], 3, kt0, accs[3], accs[3])
            for j in range(1, JW):
                weigh(ps[j], j, it, kt, False)
                gather_values(ps[j - 1], j - 1, kt, accs[j - 1], accs[j - 1])

            @pl.when((kt0 == pairs - 1) & (step > 0))
            def _():
                finish(3, it0, accs[3])

            @pl.when(kt == pairs - 1)
            def _():
                for j in range(3):
                    finish(j, it, accs[j])

            return carry

        def over_tiles_shifted(step, carry):
            j, it = step // pairs, lax.rem(step, pairs)
            mx_s[...] = jnp.full_like(mx_s, NEG)

            def highest(kt, inner):
                for h in range(H):
                    top = jnp.max(scores(j, it, kt, h), axis=-1, keepdims=True)
                    mx_s[h] = jnp.maximum(mx_s[h], top)
                return inner

            def sum_up(kt, inner):
                weigh(p0, j, it, kt, True)
                gather_values(p0, j, kt, acc0, acc0)
                return inner

            lax.fori_loop(0, pairs, highest, 0)
            lax.fori_loop(0, pairs, sum_up, 0)
            finish(j, it, acc0)
            return carry

        @pl.when(bound <= 3000.0)
        def _():
            lax.fori_loop(0, pairs * pairs, four_columns, 0)
            gather_values(ps[3], 3, pairs - 1, accs[3], accs[3])
            finish(3, pairs - 1, accs[3])

        @pl.when(jnp.logical_not(bound <= 3000.0))
        def _():
            lax.fori_loop(0, pairs * JW, over_tiles_shifted, 0)

        def write(r, carry):
            tok = pl.ds(pl.multiple_of(r * 512, 512), 512)

            @pl.when(valid_ref[r] > 0)
            def _():
                out_ref[tok, :] = (x_ref[tok, :].astype(F32) + u_s[tok, :]).astype(BF16)

            @pl.when(valid_ref[r] == 0)
            def _():
                out_ref[tok, :] = x_ref[tok, :]

            return carry

        lax.fori_loop(0, 8, write, 0)


def attend(x, bg, gain, shift, wp, gb, wo, ob, valid):
    vmem = pl.BlockSpec(memory_space=pltpu.VMEM)
    v = pltpu.VMEM
    return pl.pallas_call(
        attend_kernel,
        out_shape=jax.ShapeDtypeStruct((4096, C), BF16),
        in_specs=[pl.BlockSpec(memory_space=pltpu.SMEM), vmem, pl.BlockSpec(memory_space=pl.ANY)]
        + [vmem] * 6,
        out_specs=vmem,
        scratch_shapes=[
            v((8, 8, 2, 2, BROWS, BLK), BF16),
            v((JW, 4, H, 256, C), BF16),
            v((4, H, 256, C), BF16),
            v((JW, 1024, C), BF16),
            v((1024, C), BF16),
            v((JW, 4, H * 256, C), BF16),
            v((H * 256, C), BF16),
            v((JW, 1024, C), F32),
            v((512, C), F32), v((512, C), F32), v((512, C), F32), v((512, C), F32),
            v((256, H * 256), BF16), v((256, H * 256), BF16), v((256, H * 256), BF16), v((256, H * 256), BF16),
            v((256, 256), F32), v((256, 256), F32), v((256, 256), F32), v((256, 256), F32),
            v((4096, C), F32),
            v((H, 256, C), F32),
            v((2, 8, C), F32),
            pltpu.SMEM((16,), jnp.int32),
            pltpu.SemaphoreType.DMA((64,)),
        ],
        compiler_params=pltpu.CompilerParams(vmem_limit_bytes=60 * 1024 * 1024),
        name="attend",
    )(valid, x, bg, gain, shift, wp, gb, wo, ob)


def pass_on_kernel(y_ref, o_ref):
    o_ref[...] = y_ref[...]


def pass_on(y):
    spec = pl.BlockSpec((BLK // 4, COLS, C), lambda step: (step, 0, 0))
    return pl.pallas_call(
        pass_on_kernel,
        out_shape=jax.ShapeDtypeStruct(y.shape, y.dtype),
        grid=(4,),
        in_specs=[spec],
        out_specs=spec,
        name="pass_on",
    )(y)


def shards(pair_rep, ln_gain, ln_shift, w_proj, gate_bias, w_bias, w_out, out_bias, block_valid):
    gain, shift = ln_gain[None], ln_shift[None]
    columns, bias = exchange(pair_rep, gain, shift, w_bias.T)
    y = attend(
        columns.reshape(4096, C), bias, gain, shift, w_proj, gate_bias[None], w_out, out_bias[None],
        block_valid,
    )
    out = send_back(y.reshape(ROWS, BLK, JW, C))
    return pass_on(out.reshape(BLK, COLS, C))


def solution(mesh):
    return jax.shard_map(
        shards,
        mesh=mesh,
        in_specs=(P("row", "col", None), P(), P(), P(), P(), P(), P(), P(), P()),
        out_specs=P("row", "col", None),
        check_vma=False,
    )
```

```python
import jax
import jax.numpy as jnp
from jax import lax
from jax.experimental import pallas as pl
from jax.experimental.pallas import tpu as pltpu
from jax.sharding import PartitionSpec as P

H = 4
HD = 32
C = 128
ROWS = 8
COLS = 32
BLK = 128
JW = 4
BROWS = H * 32 + 8
COLOR_Z = (0, 64)
COLOR_Y = (64, 96)
COLOR_X = (96, 136)
MESH = pl.DeviceIdType.MESH
F32 = jnp.float32
BF16 = jnp.bfloat16
NEG = -1e30


def dot_nt(a, b):
    return lax.dot_general(a, b, (((1,), (1,)), ((), ())), preferred_element_type=F32)


def dot_nn(a, b):
    return lax.dot_general(a, b, (((1,), (0,)), ((), ())), preferred_element_type=F32)


def layer_norm(x, gain, shift):
    average = jnp.mean(x, axis=-1, keepdims=True)
    centred = x - average
    spread = jnp.mean(centred * centred, axis=-1, keepdims=True)
    return (centred * lax.rsqrt(spread + 1e-05) * gain + shift).astype(BF16)


def normalise_block(xv, gain_ref, shift_ref, n_s):
    def norm(step, carry):
        x = xv[pl.ds(step * 16, 16), :, :].astype(F32).reshape(512, C)
        n_s[pl.ds(pl.multiple_of(step * 512, 512), 512), :] = layer_norm(
            x, gain_ref[...], shift_ref[...]
        ).astype(F32)
        return carry

    lax.fori_loop(0, 8, norm, 0)


def bias_block(wb_ref, n_s, b_s, blk_ref, col):
    wide = wb_ref[...].astype(F32)
    wide = jnp.concatenate([wide, jnp.zeros((8 - H, C), F32)], axis=0).astype(BF16)
    lanes = lax.broadcasted_iota(jnp.int32, (8, BLK), 1)
    first = lax.rem(col, 4) * 32
    centres = jnp.zeros((8, BLK), F32)
    for i in range(32):
        part = dot_nt(wide, n_s[pl.ds(i, BLK, stride=32), :].astype(BF16))
        centre = jnp.max(part, axis=-1, keepdims=True).astype(BF16).astype(F32)
        part = part - centre
        for h in range(H):
            b_s[h * 32 + i : h * 32 + i + 1, :] = part[h : h + 1, :]
        centres = jnp.where(lanes == first + i, centre, centres)
    blk_ref[0 : H * 32, :] = b_s[...].astype(BF16)
    blk_ref[H * 32 :, :] = centres.astype(BF16)


class Ring:
    def __init__(self, size, mine, unit, at, send, recv):
        self.size, self.mine, self.unit, self.at, self.send, self.recv = size, mine, unit, at, send, recv
        self.last = size // 2

    def copy(self, way, step, place):
        half = way if step == self.last else None
        sign = 1 - 2 * way
        return pltpu.make_async_remote_copy(
            src_ref=self.unit(place, half),
            dst_ref=self.unit(place, half),
            send_sem=self.send.at[way, step - 1],
            recv_sem=self.recv.at[way, step - 1],
            device_id=self.at(lax.rem(self.mine + sign + self.size, self.size)),
            device_id_type=MESH,
        )

    def away(self, way, steps):
        return lax.rem(self.mine - (1 - 2 * way) * steps + self.size, self.size)

    def hop(self, way, step):
        return self.copy(way, step, self.away(way, step - 1))

    def arrival(self, way, step):
        return self.copy(way, step, self.away(way, step))


def exchange_kernel(
    x_ref, flat_ref, gain_ref, shift_ref, wb_ref, o_ref, bg_out,
    bg, xv, n_s, b_s, blk_ref, a_send, a_recv, pz_send, pz_recv, pq_send, pq_recv,
    r0s, r0r, r1s, r1r, r2s, r2r, r3s, r3r, r4s, r4r, r5s, r5r, r6s, r6r, r7s, r7r,
    r8s, r8r, r9s, r9r, ras, rar, rbs, rbr,
    dz_send, dz_recv, dy_send, dy_recv, dx_send, dx_recv, cz, cy, cx, own_sem,
):
    row = lax.axis_index("row")
    col = lax.axis_index("col")
    xl, y = row // 4, lax.rem(row, 4)
    z, xh, core = col // 4, lax.rem(col // 2, 2), lax.rem(col, 2)
    x = xh * 2 + xl
    every = slice(None)
    block_in = pltpu.make_async_copy(flat_ref, xv, own_sem.at[1])
    block_in.start()

    def device(x_, y_, z_, core_=None):
        core_ = core if core_ is None else core_
        return {"row": lax.rem(x_, 2) * 4 + y_, "col": z_ * 4 + (x_ // 2) * 2 + core_}

    rows_z = pl.ds(COLOR_Z[0], COLOR_Z[1] - COLOR_Z[0])
    rows_y = pl.ds(COLOR_Y[0], COLOR_Y[1] - COLOR_Y[0])
    rows_x = pl.ds(COLOR_X[0], COLOR_X[1] - COLOR_X[0])
    rows_q = pl.ds(COLOR_Y[0], COLOR_X[1] - COLOR_Y[0])

    def part(half, count):
        return every if half is None else pl.ds(half * count, count)

    yh, yl = y // 2, lax.rem(y, 2)

    def unit_zx(p, half):
        return bg.at[lax.rem(p, 2), part(half, 1), :, z, p // 2, rows_z, :]

    def unit_yx(p, half):
        return bg.at[lax.rem(p, 2), yh, yl, part(half, 4), p // 2, rows_y, :]

    def unit_xy(p, half):
        return bg.at[xl, p // 2, lax.rem(p, 2), part(half, 4), xh, rows_x, :]

    def unit_za(p, half):
        return bg.at[xl, part(half, 1), :, p, xh, rows_z, :]

    def unit_zb(p, half):
        return bg.at[1 - xl, part(half, 1), :, p, :, rows_z, :]

    def unit_zc(p, half):
        return bg.at[xl, part(half, 1), :, p, 1 - xh, rows_z, :]

    def unit_ya(p, half):
        return bg.at[xl, p // 2, lax.rem(p, 2), part(half, 4), xh, rows_y, :]

    def unit_yb(p, half):
        return bg.at[1 - xl, p // 2, lax.rem(p, 2), part(half, 4), :, rows_y, :]

    def unit_yc(p, half):
        return bg.at[xl, p // 2, lax.rem(p, 2), part(half, 4), 1 - xh, rows_y, :]

    def unit_xa(p, half):
        return bg.at[lax.rem(p, 2), yh, yl, part(half, 4), p // 2, rows_x, :]

    def unit_xb(p, half):
        return bg.at[lax.rem(p, 2), :, 1 - yl, part(half, 4), p // 2, rows_x, :]

    def unit_xc(p, half):
        return bg.at[lax.rem(p, 2), 1 - yh, yl, part(half, 4), p // 2, rows_x, :]

    def unit_z(p, half, ref=None, side=None):
        if ref is None:
            return bg.at[:, :, :, p, :, rows_z, :]
        return ref.at[:, :, :, p, :, side, rows_z, :]

    def unit_y(p, half, ref=None, side=None):
        if ref is None:
            return bg.at[:, p // 2, lax.rem(p, 2), :, :, rows_y, :]
        return ref.at[:, p // 2, lax.rem(p, 2), :, :, side, rows_y, :]

    def unit_x(p, half, ref=None, side=None):
        if ref is None:
            return bg.at[lax.rem(p, 2), :, :, :, p // 2, rows_x, :]
        return ref.at[lax.rem(p, 2), :, :, :, p // 2, side, rows_x, :]

    along_x = lambda p: device(p, y, z)
    along_y = lambda p: device(x, p, z)
    along_z = lambda p: device(x, y, p)
    zx = Ring(4, x, unit_zx, along_x, r0s, r0r)
    yx = Ring(4, x, unit_yx, along_x, r1s, r1r)
    xy = Ring(4, y, unit_xy, along_y, r2s, r2r)
    za = Ring(8, z, unit_za, along_z, r3s, r3r)
    zb = Ring(8, z, unit_zb, along_z, r6s, r6r)
    zc = Ring(8, z, unit_zc, along_z, r7s, r7r)
    ya = Ring(4, y, unit_ya, along_y, r4s, r4r)
    yb = Ring(4, y, unit_yb, along_y, r8s, r8r)
    yc = Ring(4, y, unit_yc, along_y, r9s, r9r)
    xa = Ring(4, x, unit_xa, along_x, r5s, r5r)
    xb = Ring(4, x, unit_xb, along_x, ras, rar)
    xc = Ring(4, x, unit_xc, along_x, rbs, rbr)
    rz = Ring(8, z, unit_z, along_z, None, None)
    ry = Ring(4, y, unit_y, along_y, None, None)
    rx = Ring(4, x, unit_x, along_x, None, None)
    finals = ((rz, dz_send, dz_recv, cz), (ry, dy_send, dy_recv, cy), (rx, dx_send, dx_recv, cx))

    def round_line(mine, size, act):
        def body(d, carry):
            act(lax.rem(mine + d, size))
            return carry

        lax.fori_loop(1, size, body, 0)

    barrier = pltpu.get_barrier_semaphore()

    def greet(target):
        pl.semaphore_signal(barrier, inc=1, device_id=target, device_id_type=MESH)

    round_line(z, 8, lambda p: greet(device(x, y, p)))
    round_line(x, 4, lambda p: greet(device(p, y, z)))
    round_line(row, ROWS, lambda p: greet({"row": p, "col": col}))
    greet(device(x, y, z, 1 - core))
    block_in.wait()
    normalise_block(xv, gain_ref, shift_ref, n_s)
    pl.semaphore_wait(barrier, 18)

    def line_z(p, sender):
        return pltpu.make_async_remote_copy(
            src_ref=blk_ref.at[rows_z, :],
            dst_ref=bg.at[xl, sender // 2, lax.rem(sender, 2), z, xh, rows_z, :],
            send_sem=pz_send.at[p],
            recv_sem=pz_recv.at[sender],
            device_id=device(x, p, z),
            device_id_type=MESH,
        )

    def line_q(p, sender):
        return pltpu.make_async_remote_copy(
            src_ref=blk_ref.at[rows_q, :],
            dst_ref=bg.at[xl, yh, yl, sender, xh, rows_q, :],
            send_sem=pq_send.at[p],
            recv_sem=pq_recv.at[sender],
            device_id=device(x, y, p),
            device_id_type=MESH,
        )


    def column(dx, dy, arriving=False):
        sign = -1 if arriving else 1
        px, py = lax.rem(xl + dx, 2), lax.rem(y + sign * dy + 4, 4)
        peer = px * 4 + py
        return pltpu.make_async_remote_copy(
            src_ref=x_ref.at[:, peer],
            dst_ref=o_ref.at[peer if arriving else row],
            send_sem=a_send.at[dx * 4 + dy],
            recv_sem=a_recv.at[dx * 4 + dy],
            device_id={"row": peer, "col": col},
            device_id_type=MESH,
        )

    keep = pltpu.make_async_copy(x_ref.at[:, row], o_ref.at[row], own_sem.at[0])
    keep.start()
    early = ()
    late = ((1, 0), (0, 1), (0, 3), (1, 1), (1, 3), (0, 2), (1, 2))
    for dx, dy in early:
        column(dx, dy).start()
    bias_block(wb_ref, n_s, b_s, blk_ref, col)
    bg[xl, yh, yl, z, xh] = blk_ref[...]
    round_line(y, 4, lambda p: line_z(p, y).start())
    round_line(z, 8, lambda p: line_q(p, z).start())

    def launch(ring, step):
        for way in (0, 1):
            ring.hop(way, step).start()

    def await_step(ring, step):
        for way in (0, 1):
            ring.arrival(way, step).wait_recv()

    def across(final, place):
        ring, send, recv, _ = final
        return pltpu.make_async_remote_copy(
            src_ref=ring.unit(place, None),
            dst_ref=ring.unit(place, None, bg_out, core),
            send_sem=send.at[place],
            recv_sem=recv.at[place],
            device_id=device(x, y, z, 1 - core),
            device_id_type=MESH,
        )

    def across_arrival(final, place):
        ring, send, recv, _ = final
        return pltpu.make_async_remote_copy(
            src_ref=ring.unit(place, None),
            dst_ref=ring.unit(place, None, bg_out, 1 - core), send_sem=send.at[place], recv_sem=recv.at[place],
            device_id=device(x, y, z, 1 - core), device_id_type=MESH,
        )

    def keep_unit(final, place):
        ring, _, _, sem = final
        return pltpu.make_async_copy(
            ring.unit(place, None), ring.unit(place, None, bg_out, core), sem.at[place]
        )

    def hand_on(final, place):
        across(final, place).start()
        keep_unit(final, place).start()

    def onward(ring, step):
        for way in (0, 1):
            ring.arrival(way, step).wait_recv()
            if step < ring.last:
                ring.hop(way, step + 1).start()

    def hand_unit(which, step):
        ring = finals[which][0]
        hand_on(finals[which], ring.away(0, step))
        if step < ring.last:
            hand_on(finals[which], ring.away(1, step))

    round_line(y, 4, lambda p: line_z(p, p).wait_recv())
    launch(zx, 1)
    launch(za, 1)
    await_step(zx, 1)
    launch(zx, 2)
    launch(zb, 1)
    round_line(z, 8, lambda p: line_q(p, p).wait_recv())
    launch(yx, 1)
    launch(xy, 1)
    launch(xa, 1)
    launch(ya, 1)
    onward(za, 1)
    await_step(zx, 2)
    launch(zc, 1)
    hand_on(finals[0], z)
    await_step(xy, 1)
    launch(xy, 2)
    launch(xb, 1)
    await_step(yx, 1)
    launch(yx, 2)
    launch(yb, 1)
    onward(zb, 1)
    await_step(xy, 2)
    launch(xc, 1)
    hand_on(finals[2], x)
    await_step(yx, 2)
    launch(yc, 1)
    hand_on(finals[1], y)
    onward(xa, 1)
    onward(ya, 1)
    onward(za, 2)
    onward(zc, 1)
    hand_unit(0, 1)
    onward(xb, 1)
    onward(yb, 1)
    onward(zb, 2)
    onward(xc, 1)
    hand_unit(2, 1)
    onward(yc, 1)
    hand_unit(1, 1)
    column(1, 0).start()
    column(0, 1).start()
    column(0, 3).start()
    column(1, 1).start()
    column(1, 3).start()
    column(0, 2).start()
    column(1, 2).start()
    onward(za, 3)
    onward(zc, 2)
    hand_unit(0, 2)
    onward(xa, 2)
    onward(xb, 2)
    onward(xc, 2)
    hand_unit(2, 2)
    onward(ya, 2)
    onward(yb, 2)
    onward(yc, 2)
    hand_unit(1, 2)
    onward(zb, 3)
    onward(za, 4)
    onward(zc, 3)
    hand_unit(0, 3)
    onward(zb, 4)
    onward(zc, 4)
    hand_unit(0, 4)

    for final in (finals[1], finals[2], finals[0]):
        ring = final[0]
        for d in range(ring.size):
            place = ring.away(d % 2, (d + 1) // 2)
            across_arrival(final, place).wait_recv()
    round_line(y, 4, lambda p: line_z(p, y).wait_send())
    round_line(z, 8, lambda p: line_q(p, z).wait_send())
    for ring in (zx, yx, xy, za, zb, zc, ya, yb, yc, xa, xb, xc):
        for way in (0, 1):
            for step in range(1, ring.last + 1):
                ring.hop(way, step).wait_send()
    for dx, dy in early + late:
        column(dx, dy).wait_send()
        column(dx, dy, True).wait_recv()
    keep.wait()
    for final in finals:
        for place in range(final[0].size):
            across(final, place).wait_send()
            keep_unit(final, place).wait()


def exchange(x, gain, shift, wb):
    dma = pltpu.SemaphoreType.DMA
    sems = [dma((8,)), dma((8,)), dma((4,)), dma((4,)), dma((8,)), dma((8,))]
    for size in (2, 2, 2, 4, 2, 2, 4, 4, 2, 2, 2, 2):
        sems += [dma((2, size)), dma((2, size))]
    sems += [dma((8,)), dma((8,)), dma((4,)), dma((4,)), dma((4,)), dma((4,))]
    sems += [dma((8,)), dma((4,)), dma((4,)), dma((2,))]
    shape = (2, 2, 2, 8, 2, 2, BROWS, BLK)
    hbm = pl.BlockSpec(memory_space=pl.ANY)
    return pl.pallas_call(
        exchange_kernel,
        out_shape=(
            jax.ShapeDtypeStruct((ROWS, BLK, JW, C), BF16),
            jax.ShapeDtypeStruct(shape, BF16),
        ),
        in_specs=[hbm, hbm] + [pl.BlockSpec(memory_space=pltpu.VMEM)] * 3,
        out_specs=(hbm, hbm),
        scratch_shapes=[
            pltpu.VMEM(shape[:5] + shape[6:], BF16),
            pltpu.VMEM((BLK, COLS, C), BF16),
            pltpu.VMEM((4096, C), F32),
            pltpu.VMEM((H * 32, BLK), F32),
            pltpu.VMEM((BROWS, BLK), BF16),
        ]
        + sems,
        compiler_params=pltpu.CompilerParams(
            collective_id=0, has_side_effects=True, vmem_limit_bytes=60 * 1024 * 1024
        ),
        name="exchange",
    )(x.reshape(BLK, ROWS, JW, C), x, gain, shift, wb)


def return_kernel(y_ref, o_ref, send, recv, local_sem):
    row = lax.axis_index("row")
    xl, y = row // 4, lax.rem(row, 4)
    barrier = pltpu.get_barrier_semaphore()
    for d in range(1, ROWS):
        pl.semaphore_signal(
            barrier, inc=1, device_id={"row": lax.rem(row + d, ROWS)}, device_id_type=MESH
        )
    keep = pltpu.make_async_copy(y_ref.at[row], o_ref.at[:, row], local_sem)
    keep.start()
    pl.semaphore_wait(barrier, ROWS - 1)

    def at(dx, dy):
        return lax.rem(xl + dx, 2) * 4 + lax.rem(y + dy + 4, 4)

    def copy(dx, dy, arriving=False):
        peer = at(dx, -dy if arriving else dy)
        return pltpu.make_async_remote_copy(
            src_ref=y_ref.at[peer],
            dst_ref=o_ref.at[:, peer if arriving else row],
            send_sem=send.at[dx * 4 + dy],
            recv_sem=recv.at[dx * 4 + dy],
            device_id={"row": peer},
            device_id_type=MESH,
        )

    ways = ((1, 2), (1, 1), (1, 3), (0, 2), (1, 0), (0, 1), (0, 3))
    for dx, dy in ways:
        copy(dx, dy).start()
    for dx, dy in ways:
        copy(dx, dy).wait_send()
        copy(dx, dy, True).wait_recv()
    keep.wait()


def send_back(y):
    dma = pltpu.SemaphoreType.DMA
    return pl.pallas_call(
        return_kernel,
        out_shape=jax.ShapeDtypeStruct((BLK, ROWS, JW, C), BF16),
        in_specs=[pl.BlockSpec(memory_space=pl.ANY)],
        out_specs=pl.BlockSpec(memory_space=pl.ANY),
        scratch_shapes=[dma((8,)), dma((8,)), dma],
        compiler_params=pltpu.CompilerParams(
            collective_id=1, has_side_effects=True, vmem_limit_bytes=60 * 1024 * 1024
        ),
        name="send_back",
    )(y)


def attend_kernel(
    valid_ref, x_ref, bg_ref, gain_ref, shift_ref, wp_ref, gb_ref, wo_ref, ob_ref, out_ref,
    bgv, q_s, e_s, k_s, kp_s, v_s, one_s, g_s, tq, tk, tv, tg, p0, p1, p2, p3, acc0, acc1, acc2, acc3, u_s, mx_s, top_s,
    idx_s, bias_sem,
):
    ps, accs = (p0, p1, p2, p3), (acc0, acc1, acc2, acc3)
    col = lax.axis_index("col")
    present = valid_ref[col // 4]

    def place(b, count):
        idx_s[count] = b
        return count + valid_ref[b]

    n = lax.fori_loop(0, 8, place, 0)
    idx_s[n] = 0
    pairs = (n + 1) // 2
    lanes = lax.broadcasted_iota(jnp.int32, (BLK, C), 1)

    def bias_copy(sk):
        rk = idx_s[sk]
        return pltpu.make_async_copy(
            bg_ref.at[rk // 4, lax.rem(rk, 4) // 2, lax.rem(rk, 2)], bgv.at[sk], bias_sem.at[sk]
        )

    @pl.when(present == 0)
    def _():
        out_ref[...] = x_ref[...]

    @pl.when(present != 0)
    def _():
        def over_blocks(act):
            def keys(sk, carry):
                act(bias_copy(sk))
                return carry

            lax.fori_loop(0, n, keys, 0)

        over_blocks(lambda copy: copy.start())
        top_s[...] = jnp.zeros_like(top_s)
        for h in range(H):
            one_s[h * 256 : (h + 1) * 256, :] = jnp.where(
                lax.broadcasted_iota(jnp.int32, (256, C), 1) // HD == h, 1.0, 0.0
            ).astype(BF16)

        def prepare(s, carry):
            r = idx_s[s]
            tok = pl.multiple_of(r * 512, 512)
            x = x_ref[pl.ds(tok, 512), :].astype(F32)
            normed = layer_norm(x, gain_ref[...], shift_ref[...])
            proj = dot_nn(normed, wp_ref[...])
            q = (proj[:, :C] * (HD ** -0.5)).astype(BF16)
            k = proj[:, C : 2 * C].astype(BF16)
            tq[...] = q.astype(F32)
            tk[...] = k.astype(F32)
            tv[...] = proj[:, 2 * C : 3 * C]
            tg[...] = jax.nn.sigmoid(proj[:, 3 * C :] + gb_ref[...])
            heads = (
                lax.broadcasted_iota(jnp.int32, (C, C), 0) // HD
                == lax.broadcasted_iota(jnp.int32, (C, C), 1) // HD
            ).astype(BF16)
            q2 = dot_nn(q * q, heads)
            k2 = dot_nn(k * k, heads)
            top_s[0] = jnp.maximum(top_s[0], jnp.max(q2.reshape(64, 8, C), axis=0))
            top_s[1] = jnp.maximum(top_s[1], jnp.max(k2.reshape(64, 8, C), axis=0))
            at = pl.multiple_of(s * BLK, BLK)
            it = s // 2
            sub = pl.multiple_of(lax.rem(s, 2) * BLK, BLK)
            for j in range(JW):
                qj = tq[pl.ds(j, BLK, stride=JW), :].astype(BF16)
                vj = tv[pl.ds(j, BLK, stride=JW), :].astype(BF16)
                k_s[j, pl.ds(at, BLK), :] = tk[pl.ds(j, BLK, stride=JW), :].astype(BF16)
                g_s[j, pl.ds(at, BLK), :] = tg[pl.ds(j, BLK, stride=JW), :]
                for h in range(H):
                    pick = one_s[h * 256 : h * 256 + BLK, :]
                    q_s[j, it, h, pl.ds(sub, BLK), :] = qj * pick
                    v_s[j, it, pl.ds(h * 256 + sub, BLK), :] = vj * pick
            kp_s[pl.ds(at, BLK), :] = jnp.where(
                (lanes // 8 == s) | (lanes // 8 == 8), 1.0, 0.0
            ).astype(BF16)
            return carry

        lax.fori_loop(0, n, prepare, 0)

        over_blocks(lambda copy: copy.wait())

        def centre(s, carry):
            r = idx_s[s]
            tiles = []
            high = jnp.full((8, BLK), NEG, F32)
            for b in range(8):
                part = bgv[b, r, 0, 0, H * 32 :, :].astype(F32)
                for q4 in range(1, 4):
                    part = part + bgv[b, r, q4 // 2, q4 % 2, H * 32 :, :].astype(F32)
                tiles.append(jnp.where(b < n, part, 0.0))
                high = jnp.maximum(high, jnp.where(b < n, part, NEG))
            tiles.append(-high)
            tiles.append(jnp.full((8, BLK), NEG, F32))
            tiles.append(jnp.zeros((48, BLK), F32))
            turned = jnp.concatenate(tiles, axis=0).T
            it = s // 2
            sub = pl.multiple_of(lax.rem(s, 2) * BLK, BLK)
            for h in range(H):
                e_s[it, h, pl.ds(sub, BLK), :] = jnp.where(
                    ((lax.rem(lanes, 8) == h) & (lanes < 72)) | (lanes == 72), turned, 0.0
                ).astype(BF16)
            return carry

        lax.fori_loop(0, n, centre, 0)

        @pl.when(lax.rem(n, 2) == 1)
        def _():
            at = pl.multiple_of(n * BLK, BLK)
            it = n // 2
            zero = jnp.zeros((BLK, C), BF16)
            kp_s[pl.ds(at, BLK), :] = jnp.where(lanes == 72, 1.0, 0.0).astype(BF16)
            for j in range(JW):
                k_s[j, pl.ds(at, BLK), :] = zero
                for h in range(H):
                    v_s[j, it, h * 256 + BLK : h * 256 + 256, :] = zero
                    q_s[j, it, h, BLK : 2 * BLK, :] = zero
            for h in range(H):
                e_s[it, h, BLK : 2 * BLK, :] = zero

        bound = jnp.max(jnp.max(top_s[0], axis=0, keepdims=True) * jnp.max(top_s[1], axis=0, keepdims=True))

        def scores(j, it, kt, h):
            keys = pl.ds(pl.multiple_of(kt * 256, 256), 256)
            s = dot_nt(
                jnp.concatenate([q_s[j, it, h], e_s[it, h]], axis=1),
                jnp.concatenate([k_s[j, keys, :], kp_s[keys, :]], axis=1),
            )
            rows = []
            for a in range(2):
                ri = idx_s[jnp.minimum(it * 2 + a, n - 1)]
                parts = []
                for b in range(2):
                    sk = jnp.minimum(kt * 2 + b, n - 1)
                    bias = bgv[sk, ri, :, :, h * 32 : h * 32 + 32, :]
                    parts.append(
                        s[a * BLK : (a + 1) * BLK, b * BLK : (b + 1) * BLK]
                        + bias.reshape(BLK, BLK).astype(F32)
                    )
                rows.append(jnp.concatenate(parts, axis=1))
            return jnp.concatenate(rows, axis=0)

        def weigh(p_ref, j, it, kt, shifted):
            for h in range(H):
                s = scores(j, it, kt, h)
                if shifted:
                    s = s - mx_s[h][:, 0:1]
                p_ref[:, h * 256 : (h + 1) * 256] = jnp.exp(s).astype(BF16)

        def gather_values(p_ref, j, kt, to_ref, from_ref):
            got = dot_nn(p_ref[...], jnp.concatenate([v_s[j, kt], one_s[...]], axis=1))
            to_ref[...] = jnp.where(kt == 0, 0.0, from_ref[...]) + got

        def finish(j, it, acc):
            base = pl.multiple_of(it * 256, 256)
            mixed = (acc[:, 0:C] / acc[:, C : 2 * C]).astype(BF16).astype(F32)
            gated = (g_s[j, pl.ds(base, 256), :] * mixed).astype(BF16)
            update = dot_nn(gated, wo_ref[...]) + ob_ref[...]
            for a in range(2):
                ri = idx_s[it * 2 + a]

                @pl.when(it * 2 + a < n)
                def _():
                    u_s[pl.ds(ri * 512 + j, BLK, stride=JW), :] = update[a * BLK : (a + 1) * BLK]

        def four_columns(it, kt):
            it0 = jnp.where(kt == 0, jnp.maximum(it - 1, 0), it)
            kt0 = jnp.where(kt == 0, pairs - 1, kt - 1)
            weigh(ps[0], 0, it, kt, False)
            gather_values(ps[3], 3, kt0, accs[3], accs[3])
            for j in range(1, JW):
                weigh(ps[j], j, it, kt, False)
                gather_values(ps[j - 1], j - 1, kt, accs[j - 1], accs[j - 1])

            @pl.when((kt == 0) & (it > 0))
            def _():
                finish(3, it0, accs[3])

            @pl.when(kt == pairs - 1)
            def _():
                for j in range(3):
                    finish(j, it, accs[j])

        def query_tiles(it, carry):
            def key_tiles(kt, inner):
                four_columns(it, kt)
                return inner

            return lax.fori_loop(0, pairs, key_tiles, carry)

        def over_tiles_shifted(step, carry):
            j, it = step // pairs, lax.rem(step, pairs)
            mx_s[...] = jnp.full_like(mx_s, NEG)

            def highest(kt, inner):
                for h in range(H):
                    top = jnp.max(scores(j, it, kt, h), axis=-1, keepdims=True)
                    mx_s[h] = jnp.maximum(mx_s[h], top)
                return inner

            def sum_up(kt, inner):
                weigh(p0, j, it, kt, True)
                gather_values(p0, j, kt, acc0, acc0)
                return inner

            lax.fori_loop(0, pairs, highest, 0)
            lax.fori_loop(0, pairs, sum_up, 0)
            finish(j, it, acc0)
            return carry

        @pl.when(bound <= 3000.0)
        def _():
            lax.fori_loop(0, pairs, query_tiles, 0)
            gather_values(ps[3], 3, pairs - 1, accs[3], accs[3])
            finish(3, pairs - 1, accs[3])

        @pl.when(jnp.logical_not(bound <= 3000.0))
        def _():
            lax.fori_loop(0, pairs * JW, over_tiles_shifted, 0)

        def write(r, carry):
            tok = pl.ds(pl.multiple_of(r * 512, 512), 512)

            @pl.when(valid_ref[r] > 0)
            def _():
                out_ref[tok, :] = (x_ref[tok, :].astype(F32) + u_s[tok, :]).astype(BF16)

            @pl.when(valid_ref[r] == 0)
            def _():
                out_ref[tok, :] = x_ref[tok, :]

            return carry

        lax.fori_loop(0, 8, write, 0)


def attend(x, bg, gain, shift, wp, gb, wo, ob, valid):
    vmem = pl.BlockSpec(memory_space=pltpu.VMEM)
    v = pltpu.VMEM
    return pl.pallas_call(
        attend_kernel,
        out_shape=jax.ShapeDtypeStruct((4096, C), BF16),
        in_specs=[pl.BlockSpec(memory_space=pltpu.SMEM), vmem, pl.BlockSpec(memory_space=pl.ANY)]
        + [vmem] * 6,
        out_specs=vmem,
        scratch_shapes=[
            v((8, 8, 2, 2, BROWS, BLK), BF16),
            v((JW, 4, H, 256, C), BF16),
            v((4, H, 256, C), BF16),
            v((JW, 1024, C), BF16),
            v((1024, C), BF16),
            v((JW, 4, H * 256, C), BF16),
            v((H * 256, C), BF16),
            v((JW, 1024, C), F32),
            v((512, C), F32), v((512, C), F32), v((512, C), F32), v((512, C), F32),
            v((256, H * 256), BF16), v((256, H * 256), BF16), v((256, H * 256), BF16), v((256, H * 256), BF16),
            v((256, 256), F32), v((256, 256), F32), v((256, 256), F32), v((256, 256), F32),
            v((4096, C), F32),
            v((H, 256, C), F32),
            v((2, 8, C), F32),
            pltpu.SMEM((16,), jnp.int32),
            pltpu.SemaphoreType.DMA((8,)),
        ],
        compiler_params=pltpu.CompilerParams(vmem_limit_bytes=60 * 1024 * 1024),
        name="attend",
    )(valid, x, bg, gain, shift, wp, gb, wo, ob)


def shards(pair_rep, ln_gain, ln_shift, w_proj, gate_bias, w_bias, w_out, out_bias, block_valid):
    gain, shift = ln_gain[None], ln_shift[None]
    columns, bias = exchange(pair_rep, gain, shift, w_bias.T)
    y = attend(
        columns.reshape(4096, C), bias, gain, shift, w_proj, gate_bias[None], w_out, out_bias[None],
        block_valid,
    )
    out = send_back(y.reshape(ROWS, BLK, JW, C))
    return out.reshape(BLK, COLS, C)


def solution(mesh):
    return jax.shard_map(
        shards,
        mesh=mesh,
        in_specs=(P("row", "col", None), P(), P(), P(), P(), P(), P(), P(), P()),
        out_specs=P("row", "col", None),
        check_vma=False,
    )
```

```python
import jax
import jax.numpy as jnp
from jax import lax
from jax.experimental import pallas as pl
from jax.experimental.pallas import tpu as pltpu
from jax.sharding import PartitionSpec as P

H = 4
HD = 32
C = 128
ROWS = 8
COLS = 32
BLK = 128
JW = 4
BROWS = H * 32 + 8
COLOR_Z = (0, 64)
COLOR_Y = (64, 96)
COLOR_X = (96, 136)
MESH = pl.DeviceIdType.MESH
F32 = jnp.float32
BF16 = jnp.bfloat16
NEG = -1e30


def dot_nt(a, b):
    return lax.dot_general(a, b, (((1,), (1,)), ((), ())), preferred_element_type=F32)


def dot_nn(a, b):
    return lax.dot_general(a, b, (((1,), (0,)), ((), ())), preferred_element_type=F32)


def layer_norm(x, gain, shift):
    average = jnp.mean(x, axis=-1, keepdims=True)
    centred = x - average
    spread = jnp.mean(centred * centred, axis=-1, keepdims=True)
    return (centred * lax.rsqrt(spread + 1e-05) * gain + shift).astype(BF16)


def normalise_block(xv, gain_ref, shift_ref, n_s):
    def norm(step, carry):
        x = xv[pl.ds(step * 16, 16), :, :].astype(F32).reshape(512, C)
        n_s[pl.ds(pl.multiple_of(step * 512, 512), 512), :] = layer_norm(
            x, gain_ref[...], shift_ref[...]
        ).astype(F32)
        return carry

    lax.fori_loop(0, 8, norm, 0)


def bias_block(wb_ref, n_s, b_s, blk_ref, col):
    wide = wb_ref[...].astype(F32)
    wide = jnp.concatenate([wide, jnp.zeros((8 - H, C), F32)], axis=0).astype(BF16)
    lanes = lax.broadcasted_iota(jnp.int32, (8, BLK), 1)
    first = lax.rem(col, 4) * 32
    centres = jnp.zeros((8, BLK), F32)
    for i in range(32):
        part = dot_nt(wide, n_s[pl.ds(i, BLK, stride=32), :].astype(BF16))
        centre = jnp.max(part, axis=-1, keepdims=True).astype(BF16).astype(F32)
        part = part - centre
        for h in range(H):
            b_s[h * 32 + i : h * 32 + i + 1, :] = part[h : h + 1, :]
        centres = jnp.where(lanes == first + i, centre, centres)
    blk_ref[0 : H * 32, :] = b_s[...].astype(BF16)
    blk_ref[H * 32 :, :] = centres.astype(BF16)


class Ring:
    def __init__(self, size, mine, unit, at, send, recv):
        self.size, self.mine, self.unit, self.at, self.send, self.recv = size, mine, unit, at, send, recv
        self.last = size // 2

    def copy(self, way, step, place):
        half = way if step == self.last else None
        sign = 1 - 2 * way
        return pltpu.make_async_remote_copy(
            src_ref=self.unit(place, half),
            dst_ref=self.unit(place, half),
            send_sem=self.send.at[way, step - 1],
            recv_sem=self.recv.at[way, step - 1],
            device_id=self.at(lax.rem(self.mine + sign + self.size, self.size)),
            device_id_type=MESH,
        )

    def away(self, way, steps):
        return lax.rem(self.mine - (1 - 2 * way) * steps + self.size, self.size)

    def hop(self, way, step):
        return self.copy(way, step, self.away(way, step - 1))

    def arrival(self, way, step):
        return self.copy(way, step, self.away(way, step))


def exchange_kernel(
    x_ref, flat_ref, gain_ref, shift_ref, wb_ref, o_ref, bg_out,
    bg, xv, n_s, b_s, blk_ref, a_send, a_recv, pz_send, pz_recv, pq_send, pq_recv,
    r0s, r0r, r1s, r1r, r2s, r2r, r3s, r3r, r4s, r4r, r5s, r5r, r6s, r6r, r7s, r7r,
    r8s, r8r, r9s, r9r, ras, rar, rbs, rbr,
    dz_send, dz_recv, dy_send, dy_recv, dx_send, dx_recv, cz, cy, cx, own_sem,
):
    row = lax.axis_index("row")
    col = lax.axis_index("col")
    xl, y = row // 4, lax.rem(row, 4)
    z, xh, core = col // 4, lax.rem(col // 2, 2), lax.rem(col, 2)
    x = xh * 2 + xl
    every = slice(None)
    block_in = pltpu.make_async_copy(flat_ref, xv, own_sem.at[1])
    block_in.start()

    def device(x_, y_, z_, core_=None):
        core_ = core if core_ is None else core_
        return {"row": lax.rem(x_, 2) * 4 + y_, "col": z_ * 4 + (x_ // 2) * 2 + core_}

    rows_z = pl.ds(COLOR_Z[0], COLOR_Z[1] - COLOR_Z[0])
    rows_y = pl.ds(COLOR_Y[0], COLOR_Y[1] - COLOR_Y[0])
    rows_x = pl.ds(COLOR_X[0], COLOR_X[1] - COLOR_X[0])
    rows_q = pl.ds(COLOR_Y[0], COLOR_X[1] - COLOR_Y[0])

    def part(half, count):
        return every if half is None else pl.ds(half * count, count)

    yh, yl = y // 2, lax.rem(y, 2)

    def unit_zx(p, half):
        return bg.at[lax.rem(p, 2), part(half, 1), :, z, p // 2, rows_z, :]

    def unit_yx(p, half):
        return bg.at[lax.rem(p, 2), yh, yl, part(half, 4), p // 2, rows_y, :]

    def unit_xy(p, half):
        return bg.at[xl, p // 2, lax.rem(p, 2), part(half, 4), xh, rows_x, :]

    def unit_za(p, half):
        return bg.at[xl, part(half, 1), :, p, xh, rows_z, :]

    def unit_zb(p, half):
        return bg.at[1 - xl, part(half, 1), :, p, :, rows_z, :]

    def unit_zc(p, half):
        return bg.at[xl, part(half, 1), :, p, 1 - xh, rows_z, :]

    def unit_ya(p, half):
        return bg.at[xl, p // 2, lax.rem(p, 2), part(half, 4), xh, rows_y, :]

    def unit_yb(p, half):
        return bg.at[1 - xl, p // 2, lax.rem(p, 2), part(half, 4), :, rows_y, :]

    def unit_yc(p, half):
        return bg.at[xl, p // 2, lax.rem(p, 2), part(half, 4), 1 - xh, rows_y, :]

    def unit_xa(p, half):
        return bg.at[lax.rem(p, 2), yh, yl, part(half, 4), p // 2, rows_x, :]

    def unit_xb(p, half):
        return bg.at[lax.rem(p, 2), :, 1 - yl, part(half, 4), p // 2, rows_x, :]

    def unit_xc(p, half):
        return bg.at[lax.rem(p, 2), 1 - yh, yl, part(half, 4), p // 2, rows_x, :]

    def unit_z(p, half, ref=None, side=None):
        if ref is None:
            return bg.at[:, :, :, p, :, rows_z, :]
        return ref.at[:, :, :, p, :, side, rows_z, :]

    def unit_y(p, half, ref=None, side=None):
        if ref is None:
            return bg.at[:, p // 2, lax.rem(p, 2), :, :, rows_y, :]
        return ref.at[:, p // 2, lax.rem(p, 2), :, :, side, rows_y, :]

    def unit_x(p, half, ref=None, side=None):
        if ref is None:
            return bg.at[lax.rem(p, 2), :, :, :, p // 2, rows_x, :]
        return ref.at[lax.rem(p, 2), :, :, :, p // 2, side, rows_x, :]

    along_x = lambda p: device(p, y, z)
    along_y = lambda p: device(x, p, z)
    along_z = lambda p: device(x, y, p)
    zx = Ring(4, x, unit_zx, along_x, r0s, r0r)
    yx = Ring(4, x, unit_yx, along_x, r1s, r1r)
    xy = Ring(4, y, unit_xy, along_y, r2s, r2r)
    za = Ring(8, z, unit_za, along_z, r3s, r3r)
    zb = Ring(8, z, unit_zb, along_z, r6s, r6r)
    zc = Ring(8, z, unit_zc, along_z, r7s, r7r)
    ya = Ring(4, y, unit_ya, along_y, r4s, r4r)
    yb = Ring(4, y, unit_yb, along_y, r8s, r8r)
    yc = Ring(4, y, unit_yc, along_y, r9s, r9r)
    xa = Ring(4, x, unit_xa, along_x, r5s, r5r)
    xb = Ring(4, x, unit_xb, along_x, ras, rar)
    xc = Ring(4, x, unit_xc, along_x, rbs, rbr)
    rz = Ring(8, z, unit_z, along_z, None, None)
    ry = Ring(4, y, unit_y, along_y, None, None)
    rx = Ring(4, x, unit_x, along_x, None, None)
    finals = ((rz, dz_send, dz_recv, cz), (ry, dy_send, dy_recv, cy), (rx, dx_send, dx_recv, cx))

    def round_line(mine, size, act):
        def body(d, carry):
            act(lax.rem(mine + d, size))
            return carry

        lax.fori_loop(1, size, body, 0)

    barrier = pltpu.get_barrier_semaphore()

    def greet(target):
        pl.semaphore_signal(barrier, inc=1, device_id=target, device_id_type=MESH)

    round_line(z, 8, lambda p: greet(device(x, y, p)))
    round_line(x, 4, lambda p: greet(device(p, y, z)))
    round_line(row, ROWS, lambda p: greet({"row": p, "col": col}))
    greet(device(x, y, z, 1 - core))
    block_in.wait()
    normalise_block(xv, gain_ref, shift_ref, n_s)
    pl.semaphore_wait(barrier, 18)

    def line_z(p, sender):
        return pltpu.make_async_remote_copy(
            src_ref=blk_ref.at[rows_z, :],
            dst_ref=bg.at[xl, sender // 2, lax.rem(sender, 2), z, xh, rows_z, :],
            send_sem=pz_send.at[p],
            recv_sem=pz_recv.at[sender],
            device_id=device(x, p, z),
            device_id_type=MESH,
        )

    def line_q(p, sender):
        return pltpu.make_async_remote_copy(
            src_ref=blk_ref.at[rows_q, :],
            dst_ref=bg.at[xl, yh, yl, sender, xh, rows_q, :],
            send_sem=pq_send.at[p],
            recv_sem=pq_recv.at[sender],
            device_id=device(x, y, p),
            device_id_type=MESH,
        )


    def column(dx, dy, arriving=False):
        sign = -1 if arriving else 1
        px, py = lax.rem(xl + dx, 2), lax.rem(y + sign * dy + 4, 4)
        peer = px * 4 + py
        return pltpu.make_async_remote_copy(
            src_ref=x_ref.at[:, peer],
            dst_ref=o_ref.at[peer if arriving else row],
            send_sem=a_send.at[dx * 4 + dy],
            recv_sem=a_recv.at[dx * 4 + dy],
            device_id={"row": peer, "col": col},
            device_id_type=MESH,
        )

    keep = pltpu.make_async_copy(x_ref.at[:, row], o_ref.at[row], own_sem.at[0])
    keep.start()
    early = ()
    late = ((1, 0), (0, 1), (0, 3), (1, 1), (1, 3), (0, 2), (1, 2))
    for dx, dy in early:
        column(dx, dy).start()
    bias_block(wb_ref, n_s, b_s, blk_ref, col)
    bg[xl, yh, yl, z, xh] = blk_ref[...]
    round_line(y, 4, lambda p: line_z(p, y).start())
    round_line(z, 8, lambda p: line_q(p, z).start())

    def launch(ring, step):
        for way in (0, 1):
            ring.hop(way, step).start()

    def await_step(ring, step):
        for way in (0, 1):
            ring.arrival(way, step).wait_recv()

    def across(final, place):
        ring, send, recv, _ = final
        return pltpu.make_async_remote_copy(
            src_ref=ring.unit(place, None),
            dst_ref=ring.unit(place, None, bg_out, core),
            send_sem=send.at[place],
            recv_sem=recv.at[place],
            device_id=device(x, y, z, 1 - core),
            device_id_type=MESH,
        )

    def across_arrival(final, place):
        ring, send, recv, _ = final
        return pltpu.make_async_remote_copy(
            src_ref=ring.unit(place, None),
            dst_ref=ring.unit(place, None, bg_out, 1 - core), send_sem=send.at[place], recv_sem=recv.at[place],
            device_id=device(x, y, z, 1 - core), device_id_type=MESH,
        )

    def keep_unit(final, place):
        ring, _, _, sem = final
        return pltpu.make_async_copy(
            ring.unit(place, None), ring.unit(place, None, bg_out, core), sem.at[place]
        )

    def hand_on(final, place):
        across(final, place).start()
        keep_unit(final, place).start()

    def onward(ring, step):
        for way in (0, 1):
            ring.arrival(way, step).wait_recv()
            if step < ring.last:
                ring.hop(way, step + 1).start()

    def hand_unit(which, step):
        ring = finals[which][0]
        hand_on(finals[which], ring.away(0, step))
        if step < ring.last:
            hand_on(finals[which], ring.away(1, step))

    round_line(y, 4, lambda p: line_z(p, p).wait_recv())
    launch(zx, 1)
    launch(za, 1)
    await_step(zx, 1)
    launch(zx, 2)
    launch(zb, 1)
    round_line(z, 8, lambda p: line_q(p, p).wait_recv())
    launch(yx, 1)
    launch(xy, 1)
    launch(xa, 1)
    launch(ya, 1)
    onward(za, 1)
    await_step(zx, 2)
    launch(zc, 1)
    hand_on(finals[0], z)
    await_step(xy, 1)
    launch(xy, 2)
    launch(xb, 1)
    await_step(yx, 1)
    launch(yx, 2)
    launch(yb, 1)
    onward(zb, 1)
    await_step(xy, 2)
    launch(xc, 1)
    hand_on(finals[2], x)
    await_step(yx, 2)
    launch(yc, 1)
    hand_on(finals[1], y)
    onward(xa, 1)
    onward(ya, 1)
    onward(za, 2)
    onward(zc, 1)
    hand_unit(0, 1)
    onward(xb, 1)
    onward(yb, 1)
    onward(zb, 2)
    onward(xc, 1)
    hand_unit(2, 1)
    onward(yc, 1)
    hand_unit(1, 1)
    column(1, 0).start()
    column(0, 1).start()
    column(0, 3).start()
    column(1, 1).start()
    column(1, 3).start()
    column(0, 2).start()
    column(1, 2).start()
    onward(za, 3)
    onward(zc, 2)
    hand_unit(0, 2)
    onward(xa, 2)
    onward(xb, 2)
    onward(xc, 2)
    hand_unit(2, 2)
    onward(ya, 2)
    onward(yb, 2)
    onward(yc, 2)
    hand_unit(1, 2)
    onward(zb, 3)
    onward(za, 4)
    onward(zc, 3)
    hand_unit(0, 3)
    onward(zb, 4)
    onward(zc, 4)
    hand_unit(0, 4)

    for final in (finals[1], finals[2], finals[0]):
        ring = final[0]
        for d in range(ring.size):
            place = ring.away(d % 2, (d + 1) // 2)
            across_arrival(final, place).wait_recv()
    round_line(y, 4, lambda p: line_z(p, y).wait_send())
    round_line(z, 8, lambda p: line_q(p, z).wait_send())
    for ring in (zx, yx, xy, za, zb, zc, ya, yb, yc, xa, xb, xc):
        for way in (0, 1):
            for step in range(1, ring.last + 1):
                ring.hop(way, step).wait_send()
    for dx, dy in early + late:
        column(dx, dy).wait_send()
        column(dx, dy, True).wait_recv()
    keep.wait()
    for final in finals:
        for place in range(final[0].size):
            across(final, place).wait_send()
            keep_unit(final, place).wait()


def exchange(x, gain, shift, wb):
    dma = pltpu.SemaphoreType.DMA
    sems = [dma((8,)), dma((8,)), dma((4,)), dma((4,)), dma((8,)), dma((8,))]
    for size in (2, 2, 2, 4, 2, 2, 4, 4, 2, 2, 2, 2):
        sems += [dma((2, size)), dma((2, size))]
    sems += [dma((8,)), dma((8,)), dma((4,)), dma((4,)), dma((4,)), dma((4,))]
    sems += [dma((8,)), dma((4,)), dma((4,)), dma((2,))]
    shape = (2, 2, 2, 8, 2, 2, BROWS, BLK)
    hbm = pl.BlockSpec(memory_space=pl.ANY)
    return pl.pallas_call(
        exchange_kernel,
        out_shape=(
            jax.ShapeDtypeStruct((ROWS, BLK, JW, C), BF16),
            jax.ShapeDtypeStruct(shape, BF16),
        ),
        in_specs=[hbm, hbm] + [pl.BlockSpec(memory_space=pltpu.VMEM)] * 3,
        out_specs=(hbm, hbm),
        scratch_shapes=[
            pltpu.VMEM(shape[:5] + shape[6:], BF16),
            pltpu.VMEM((BLK, COLS, C), BF16),
            pltpu.VMEM((4096, C), F32),
            pltpu.VMEM((H * 32, BLK), F32),
            pltpu.VMEM((BROWS, BLK), BF16),
        ]
        + sems,
        compiler_params=pltpu.CompilerParams(
            collective_id=0, has_side_effects=True, vmem_limit_bytes=60 * 1024 * 1024
        ),
        name="exchange",
    )(x.reshape(BLK, ROWS, JW, C), x, gain, shift, wb)


def return_kernel(y_ref, o_ref, send, recv, local_sem):
    row = lax.axis_index("row")
    xl, y = row // 4, lax.rem(row, 4)
    barrier = pltpu.get_barrier_semaphore()
    for d in range(1, ROWS):
        pl.semaphore_signal(
            barrier, inc=1, device_id={"row": lax.rem(row + d, ROWS)}, device_id_type=MESH
        )
    keep = pltpu.make_async_copy(y_ref.at[row], o_ref.at[:, row], local_sem)
    keep.start()
    pl.semaphore_wait(barrier, ROWS - 1)

    def at(dx, dy):
        return lax.rem(xl + dx, 2) * 4 + lax.rem(y + dy + 4, 4)

    def copy(dx, dy, arriving=False):
        peer = at(dx, -dy if arriving else dy)
        return pltpu.make_async_remote_copy(
            src_ref=y_ref.at[peer],
            dst_ref=o_ref.at[:, peer if arriving else row],
            send_sem=send.at[dx * 4 + dy],
            recv_sem=recv.at[dx * 4 + dy],
            device_id={"row": peer},
            device_id_type=MESH,
        )

    ways = ((1, 2), (1, 1), (1, 3), (0, 2), (1, 0), (0, 1), (0, 3))
    for dx, dy in ways:
        copy(dx, dy).start()
    for dx, dy in ways:
        copy(dx, dy).wait_send()
        copy(dx, dy, True).wait_recv()
    keep.wait()


def send_back(y):
    dma = pltpu.SemaphoreType.DMA
    return pl.pallas_call(
        return_kernel,
        out_shape=jax.ShapeDtypeStruct((BLK, ROWS, JW, C), BF16),
        in_specs=[pl.BlockSpec(memory_space=pl.ANY)],
        out_specs=pl.BlockSpec(memory_space=pl.ANY),
        scratch_shapes=[dma((8,)), dma((8,)), dma],
        compiler_params=pltpu.CompilerParams(
            collective_id=1, has_side_effects=True, vmem_limit_bytes=60 * 1024 * 1024
        ),
        name="send_back",
    )(y)


def attend_kernel(
    valid_ref, x_ref, bg_ref, gain_ref, shift_ref, wp_ref, gb_ref, wo_ref, ob_ref, out_ref,
    bgv, q_s, e_s, k_s, kp_s, v_s, one_s, g_s, tq, tk, tv, tg, p0, p1, p2, p3, acc0, acc1, acc2, acc3, u_s, mx_s, top_s,
    idx_s, bias_sem,
):
    ps, accs = (p0, p1, p2, p3), (acc0, acc1, acc2, acc3)
    col = lax.axis_index("col")
    present = valid_ref[col // 4]

    def place(b, count):
        idx_s[count] = b
        return count + valid_ref[b]

    n = lax.fori_loop(0, 8, place, 0)
    idx_s[n] = lax.fori_loop(0, 8, lambda b, at: jnp.where(valid_ref[b] == 0, b, at), 0)
    pairs = (n + 1) // 2
    lanes = lax.broadcasted_iota(jnp.int32, (BLK, C), 1)

    def bias_copy(sk):
        rk = idx_s[sk]
        return pltpu.make_async_copy(
            bg_ref.at[rk // 4, lax.rem(rk, 4) // 2, lax.rem(rk, 2)], bgv.at[sk], bias_sem.at[sk]
        )

    @pl.when(present == 0)
    def _():
        out_ref[...] = x_ref[...]

    @pl.when(present != 0)
    def _():
        def over_blocks(act):
            def keys(sk, carry):
                act(bias_copy(sk))
                return carry

            lax.fori_loop(0, n, keys, 0)

        over_blocks(lambda copy: copy.start())
        top_s[...] = jnp.zeros_like(top_s)
        for h in range(H):
            one_s[h * 256 : (h + 1) * 256, :] = jnp.where(
                lax.broadcasted_iota(jnp.int32, (256, C), 1) // HD == h, 1.0, 0.0
            ).astype(BF16)

        def prepare(s, carry):
            r = idx_s[s]
            tok = pl.multiple_of(r * 512, 512)
            x = x_ref[pl.ds(tok, 512), :].astype(F32)
            normed = layer_norm(x, gain_ref[...], shift_ref[...])
            proj = dot_nn(normed, wp_ref[...])
            q = (proj[:, :C] * (HD ** -0.5)).astype(BF16)
            k = proj[:, C : 2 * C].astype(BF16)
            tq[...] = q.astype(F32)
            tk[...] = k.astype(F32)
            tv[...] = proj[:, 2 * C : 3 * C]
            tg[...] = jax.nn.sigmoid(proj[:, 3 * C :] + gb_ref[...])
            heads = (
                lax.broadcasted_iota(jnp.int32, (C, C), 0) // HD
                == lax.broadcasted_iota(jnp.int32, (C, C), 1) // HD
            ).astype(BF16)
            q2 = dot_nn(q * q, heads)
            k2 = dot_nn(k * k, heads)
            top_s[0] = jnp.maximum(top_s[0], jnp.max(q2.reshape(64, 8, C), axis=0))
            top_s[1] = jnp.maximum(top_s[1], jnp.max(k2.reshape(64, 8, C), axis=0))
            at = pl.multiple_of(s * BLK, BLK)
            it = s // 2
            sub = pl.multiple_of(lax.rem(s, 2) * BLK, BLK)
            for j in range(JW):
                qj = tq[pl.ds(j, BLK, stride=JW), :].astype(BF16)
                vj = tv[pl.ds(j, BLK, stride=JW), :].astype(BF16)
                k_s[j, pl.ds(at, BLK), :] = tk[pl.ds(j, BLK, stride=JW), :].astype(BF16)
                g_s[j, pl.ds(at, BLK), :] = tg[pl.ds(j, BLK, stride=JW), :]
                for h in range(H):
                    pick = one_s[h * 256 : h * 256 + BLK, :]
                    q_s[j, it, h, pl.ds(sub, BLK), :] = qj * pick
                    v_s[j, it, pl.ds(h * 256 + sub, BLK), :] = vj * pick
            kp_s[pl.ds(at, BLK), :] = jnp.where(
                (lanes // 8 == s) | (lanes // 8 == 8), 1.0, 0.0
            ).astype(BF16)
            return carry

        lax.fori_loop(0, n, prepare, 0)

        over_blocks(lambda copy: copy.wait())

        def centre(s, carry):
            r = idx_s[s]
            tiles = []
            high = jnp.full((8, BLK), NEG, F32)
            for b in range(8):
                part = bgv[b, r, 0, 0, H * 32 :, :].astype(F32)
                for q4 in range(1, 4):
                    part = part + bgv[b, r, q4 // 2, q4 % 2, H * 32 :, :].astype(F32)
                tiles.append(jnp.where(b < n, part, 0.0))
                high = jnp.maximum(high, jnp.where(b < n, part, NEG))
            tiles.append(-high)
            tiles.append(jnp.full((8, BLK), NEG, F32))
            tiles.append(jnp.zeros((48, BLK), F32))
            turned = jnp.concatenate(tiles, axis=0).T
            it = s // 2
            sub = pl.multiple_of(lax.rem(s, 2) * BLK, BLK)
            for h in range(H):
                e_s[it, h, pl.ds(sub, BLK), :] = jnp.where(
                    ((lax.rem(lanes, 8) == h) & (lanes < 72)) | (lanes == 72), turned, 0.0
                ).astype(BF16)
            return carry

        lax.fori_loop(0, n, centre, 0)

        @pl.when(lax.rem(n, 2) == 1)
        def _():
            at = pl.multiple_of(n * BLK, BLK)
            it = n // 2
            zero = jnp.zeros((BLK, C), BF16)
            kp_s[pl.ds(at, BLK), :] = jnp.where(lanes == 72, 1.0, 0.0).astype(BF16)
            for j in range(JW):
                k_s[j, pl.ds(at, BLK), :] = zero
                for h in range(H):
                    v_s[j, it, h * 256 + BLK : h * 256 + 256, :] = zero
                    q_s[j, it, h, BLK : 2 * BLK, :] = zero
            for h in range(H):
                e_s[it, h, BLK : 2 * BLK, :] = zero

        bound = jnp.max(jnp.max(top_s[0], axis=0, keepdims=True) * jnp.max(top_s[1], axis=0, keepdims=True))

        def scores(j, it, kt, h):
            keys = pl.ds(pl.multiple_of(kt * 256, 256), 256)
            s = dot_nt(
                jnp.concatenate([q_s[j, it, h], e_s[it, h]], axis=1),
                jnp.concatenate([k_s[j, keys, :], kp_s[keys, :]], axis=1),
            )
            rows = []
            for a in range(2):
                ri = idx_s[jnp.minimum(it * 2 + a, n - 1)]
                parts = []
                for b in range(2):
                    sk = jnp.minimum(kt * 2 + b, n - 1)
                    bias = bgv[sk, ri, :, :, h * 32 : h * 32 + 32, :]
                    parts.append(
                        s[a * BLK : (a + 1) * BLK, b * BLK : (b + 1) * BLK]
                        + bias.reshape(BLK, BLK).astype(F32)
                    )
                rows.append(jnp.concatenate(parts, axis=1))
            return jnp.concatenate(rows, axis=0)

        def weigh(p_ref, j, it, kt, shifted):
            for h in range(H):
                s = scores(j, it, kt, h)
                if shifted:
                    s = s - mx_s[h][:, 0:1]
                p_ref[:, h * 256 : (h + 1) * 256] = jnp.exp(s).astype(BF16)

        def gather_values(p_ref, j, kt, to_ref, from_ref):
            got = dot_nn(p_ref[...], jnp.concatenate([v_s[j, kt], one_s[...]], axis=1))
            to_ref[...] = jnp.where(kt == 0, 0.0, from_ref[...]) + got

        def finish(j, it, acc):
            base = pl.multiple_of(it * 256, 256)
            mixed = (acc[:, 0:C] / acc[:, C : 2 * C]).astype(BF16).astype(F32)
            gated = (g_s[j, pl.ds(base, 256), :] * mixed).astype(BF16)
            update = dot_nn(gated, wo_ref[...]) + ob_ref[...]
            for a in range(2):
                ri = idx_s[it * 2 + a]
                u_s[pl.ds(ri * 512 + j, BLK, stride=JW), :] = update[a * BLK : (a + 1) * BLK]

        def four_columns(it, kt):
            it0 = jnp.where(kt == 0, jnp.maximum(it - 1, 0), it)
            kt0 = jnp.where(kt == 0, pairs - 1, kt - 1)
            weigh(ps[0], 0, it, kt, False)
            gather_values(ps[3], 3, kt0, accs[3], accs[3])
            for j in range(1, JW):
                weigh(ps[j], j, it, kt, False)
                gather_values(ps[j - 1], j - 1, kt, accs[j - 1], accs[j - 1])

            @pl.when((kt == 0) & (it > 0))
            def _():
                finish(3, it0, accs[3])

            @pl.when(kt == pairs - 1)
            def _():
                for j in range(3):
                    finish(j, it, accs[j])

        def query_tiles(it, carry):
            def key_tiles(kt, inner):
                four_columns(it, kt)
                return inner

            return lax.fori_loop(0, pairs, key_tiles, carry)

        def over_tiles_shifted(step, carry):
            j, it = step // pairs, lax.rem(step, pairs)
            mx_s[...] = jnp.full_like(mx_s, NEG)

            def highest(kt, inner):
                for h in range(H):
                    top = jnp.max(scores(j, it, kt, h), axis=-1, keepdims=True)
                    mx_s[h] = jnp.maximum(mx_s[h], top)
                return inner

            def sum_up(kt, inner):
                weigh(p0, j, it, kt, True)
                gather_values(p0, j, kt, acc0, acc0)
                return inner

            lax.fori_loop(0, pairs, highest, 0)
            lax.fori_loop(0, pairs, sum_up, 0)
            finish(j, it, acc0)
            return carry

        @pl.when(bound <= 3000.0)
        def _():
            lax.fori_loop(0, pairs, query_tiles, 0)
            gather_values(ps[3], 3, pairs - 1, accs[3], accs[3])
            finish(3, pairs - 1, accs[3])

        @pl.when(jnp.logical_not(bound <= 3000.0))
        def _():
            lax.fori_loop(0, pairs * JW, over_tiles_shifted, 0)

        def write(r, carry):
            tok = pl.ds(pl.multiple_of(r * 512, 512), 512)

            @pl.when(valid_ref[r] > 0)
            def _():
                out_ref[tok, :] = (x_ref[tok, :].astype(F32) + u_s[tok, :]).astype(BF16)

            @pl.when(valid_ref[r] == 0)
            def _():
                out_ref[tok, :] = x_ref[tok, :]

            return carry

        lax.fori_loop(0, 8, write, 0)


def attend(x, bg, gain, shift, wp, gb, wo, ob, valid):
    vmem = pl.BlockSpec(memory_space=pltpu.VMEM)
    v = pltpu.VMEM
    return pl.pallas_call(
        attend_kernel,
        out_shape=jax.ShapeDtypeStruct((4096, C), BF16),
        in_specs=[pl.BlockSpec(memory_space=pltpu.SMEM), vmem, pl.BlockSpec(memory_space=pl.ANY)]
        + [vmem] * 6,
        out_specs=vmem,
        scratch_shapes=[
            v((8, 8, 2, 2, BROWS, BLK), BF16),
            v((JW, 4, H, 256, C), BF16),
            v((4, H, 256, C), BF16),
            v((JW, 1024, C), BF16),
            v((1024, C), BF16),
            v((JW, 4, H * 256, C), BF16),
            v((H * 256, C), BF16),
            v((JW, 1024, C), F32),
            v((512, C), F32), v((512, C), F32), v((512, C), F32), v((512, C), F32),
            v((256, H * 256), BF16), v((256, H * 256), BF16), v((256, H * 256), BF16), v((256, H * 256), BF16),
            v((256, 256), F32), v((256, 256), F32), v((256, 256), F32), v((256, 256), F32),
            v((4096, C), F32),
            v((H, 256, C), F32),
            v((2, 8, C), F32),
            pltpu.SMEM((16,), jnp.int32),
            pltpu.SemaphoreType.DMA((8,)),
        ],
        compiler_params=pltpu.CompilerParams(vmem_limit_bytes=60 * 1024 * 1024),
        name="attend",
    )(valid, x, bg, gain, shift, wp, gb, wo, ob)


def shards(pair_rep, ln_gain, ln_shift, w_proj, gate_bias, w_bias, w_out, out_bias, block_valid):
    gain, shift = ln_gain[None], ln_shift[None]
    columns, bias = exchange(pair_rep, gain, shift, w_bias.T)
    y = attend(
        columns.reshape(4096, C), bias, gain, shift, w_proj, gate_bias[None], w_out, out_bias[None],
        block_valid,
    )
    out = send_back(y.reshape(ROWS, BLK, JW, C))
    return out.reshape(BLK, COLS, C)


def solution(mesh):
    return jax.shard_map(
        shards,
        mesh=mesh,
        in_specs=(P("row", "col", None), P(), P(), P(), P(), P(), P(), P(), P()),
        out_specs=P("row", "col", None),
        check_vma=False,
    )
```
